8 devices in a mesh: dp: 2 (over y, z), sp: 4 (over x, core).
Axes of the slice: x: 2, y: 2, z: 1, core: 2. Of those that a mesh axis runs over, the one named last changes fastest.
Arguments:
- x: bfloat16 [4096, 3072], P(('dp', 'sp')), parts along dimension 0
- gain: bfloat16 [3072], replicated
- wq: bfloat16 [3072, 3072], replicated
- wk: bfloat16 [3072, 1024], replicated
- wv: bfloat16 [3072, 1024], replicated
- wo: bfloat16 [3072, 3072], replicated
Outputs:
- output: bfloat16 [4096, 3072], P(('dp', 'sp')), parts along dimension 0
There are 2 independent parts. The reference program is written for one: setup_inputs(seed, part) draws one part's arguments, and reference() takes and returns one part's arrays. A program takes and returns all parts, laid end to end along the dimension named above; an argument that names none is the same for every part.
All inputs are finite; a program needn't handle non-finite values.
Results may differ from the reference program's by a relative error of at most 0.012.
Values are sent between devices in bfloat16 or wider.
A program may use at most 2 GiB of HBM per device.

```python
import jax
import jax.numpy as jnp
from jax import lax

ROWS = 2048
D = 3072
HEADS = 24
KV_HEADS = 8
HEAD = 128
THETA = 10000


def setup_inputs(seed: int = 0, part: int = 0) -> dict:
    kx, kn, kq, kk, kv, ko = jax.random.split(jax.random.key(seed), 6)

    def weights(key, rows, columns):
        return jax.random.normal(key, (rows, columns), jnp.float32) * rows**-0.5

    drawn = {
        "x": jax.random.normal(jax.random.fold_in(kx, part), (ROWS, D), jnp.float32),
        "gain": 1 + 0.1 * jax.random.normal(kn, (D,), jnp.float32),
        "wq": 2 * weights(kq, D, HEADS * HEAD),
        "wk": 2 * weights(kk, D, KV_HEADS * HEAD),
        "wv": 4 * weights(kv, D, KV_HEADS * HEAD),
        "wo": weights(ko, HEADS * HEAD, D),
    }
    return {k: v.astype(jnp.bfloat16) for k, v in drawn.items()}


def normed(x, gain):
    wide = x.astype(jnp.float32)
    scale = lax.rsqrt(jnp.mean(wide * wide, -1, keepdims=True) + 1e-6)
    return (wide * scale * gain.astype(jnp.float32)).astype(jnp.bfloat16)


def turned(t, place, theta):
    half = t.shape[-1] // 2
    angle = place.astype(jnp.float32)[:, None] * theta ** (-jnp.arange(half, dtype=jnp.float32) / half)
    cos, sin = jnp.cos(angle)[:, None], jnp.sin(angle)[:, None]
    a, b = t[..., :half].astype(jnp.float32), t[..., half:].astype(jnp.float32)
    return jnp.concatenate([a * cos - b * sin, b * cos + a * sin], -1).astype(jnp.bfloat16)


def matmul(a, w):
    return jnp.dot(a, w, preferred_element_type=jnp.float32).astype(jnp.bfloat16)


def einsum(form, a, b):
    return jnp.einsum(form, a.astype(jnp.float32), b.astype(jnp.float32))


def attention(q, k, v):
    scores = einsum("tgsd,ugd->gstu", q, k) * q.shape[-1] ** -0.5
    token = jnp.arange(q.shape[0])
    scores = jnp.where(token[:, None] >= token, scores, -jnp.inf)
    weights = jax.nn.softmax(scores, -1).astype(jnp.bfloat16)
    return einsum("gstu,ugd->tgsd", weights, v).astype(jnp.bfloat16)


def reference(x, gain, wq, wk, wv, wo):
    a, place = normed(x, gain), jnp.arange(ROWS)
    q = turned(matmul(a, wq).reshape(ROWS, HEADS, HEAD), place, THETA).reshape(ROWS, KV_HEADS, -1, HEAD)
    k = turned(matmul(a, wk).reshape(ROWS, KV_HEADS, HEAD), place, THETA)
    v = matmul(a, wv).reshape(ROWS, KV_HEADS, HEAD)
    seen = attention(q, k, v).reshape(ROWS, HEADS * HEAD)
    return (x.astype(jnp.float32) + jnp.dot(seen, wo, preferred_element_type=jnp.float32)).astype(jnp.bfloat16)
```

```python
import functools

import jax
import jax.numpy as jnp
import numpy as np
from jax import lax
from jax.experimental import pallas as pl
from jax.experimental.pallas import tpu as pltpu
from jax.sharding import PartitionSpec as P

HEAD = 128
HEADS = 24
KV = 8
D = 3072
T = 512
THETA = 10000
LOG2E = 1.4426950408889634
E = HEAD**-0.5 * LOG2E
PAIRS = KV // 2
GROUP = HEADS // KV
CHUNK = 512
MESH = pl.DeviceIdType.MESH
F32, BF16 = jnp.float32, jnp.bfloat16


def _dot(a, b, ca, cb):
    return lax.dot_general(a, b, (((ca,), (cb,)), ((), ())), preferred_element_type=F32)


def _table(rows):
    half = HEAD // 2
    rate = np.float32(THETA) ** (-np.arange(half, dtype=np.float32) / np.float32(half))
    angle = (np.arange(rows, dtype=np.float32)[:, None] * rate.astype(np.float32)).astype(np.float64)
    return np.concatenate([np.cos(angle), np.sin(angle)], 1).astype(np.float32)


def _kernel(x_hbm, gain_ref, tab_hbm, wq, wk, wv, wo, out_hbm, x_v, a_v, tab_v, cos_v, sin_v, w_v, wo_v, q_s, k_s, v_s, top_s, mix_s, o_s, y_s,
            x_sem, tab_sem, w_sem, wo_sem, out_sem, link_sem, near_sem, hand_sem, recv_sem):
    me = lax.axis_index("sp")

    rows = T // 4
    x_copies = [pltpu.make_async_copy(x_hbm.at[pl.ds(i * rows, rows)], x_v.at[pl.ds(i * rows, rows)], x_sem.at[i]) for i in range(4)]
    tab_copy = pltpu.make_async_copy(tab_hbm.at[pl.ds(pl.multiple_of(me * T, T), T)], tab_v, tab_sem)

    def weights(w, i, slot):
        return pltpu.make_async_copy(w.at[:, pl.ds(pl.multiple_of(i * 256, 256), 256)], w_v.at[slot], w_sem.at[slot])

    def out_weights(p):
        slot = lax.rem(p, 2)
        rows = GROUP * 2 * HEAD
        return pltpu.make_async_copy(wo.at[pl.ds(pl.multiple_of(p * rows, rows), rows)], wo_v.at[slot], wo_sem.at[slot])

    for c in x_copies:
        c.start()
    weights(wk, 0, 0).start()
    weights(wv, 0, 1).start()
    tab_copy.start()
    weights(wk, 1, 2).start()
    weights(wv, 1, 3).start()

    barrier = pltpu.get_barrier_semaphore()
    for i in range(1, 4):
        pl.semaphore_signal(barrier, inc=1, device_id={"sp": lax.rem(me + i, 4)}, device_id_type=MESH)

    def move(src, p, kv, send, to):
        buf = (k_s, v_s)[kv]
        part = buf.at[src, pl.ds(2 * p, 2)]
        return pltpu.make_async_remote_copy(part, part, send_sem=send, recv_sem=recv_sem.at[src, p, kv], device_id={"sp": to}, device_id_type=MESH)

    def link(p, kv):
        return move(me, p, kv, link_sem.at[p, kv], 2)

    def near(p, kv):
        return move(me, p, kv, near_sem.at[p, kv], lax.rem(me + 1, 4))

    def hand(src, p, kv):
        return move(src, p, kv, hand_sem.at[src, p, kv], 3)

    def send(p, kv):
        @pl.when(me < 2)
        def _():
            link(p, kv).start()

        @pl.when(lax.rem(me, 2) == 0)
        def _():
            near(p, kv).start()

    for i, c in enumerate(x_copies):
        c.wait()
        here = pl.ds(i * rows, rows)
        total = jnp.zeros((rows, 128), F32)
        for at in range(0, D, 128):
            t = x_v[here, at : at + 128].astype(F32)
            total += t * t
        scale = lax.rsqrt(jnp.sum(total, 1, keepdims=True) * (1 / D) + 1e-6)
        for at in range(0, D, 128):
            t = x_v[here, at : at + 128].astype(F32)
            a_v[here, at : at + 128] = (t * scale * gain_ref[:, at : at + 128].astype(F32)).astype(BF16)

    tab_copy.wait()
    tab = tab_v[...]
    other = pltpu.roll(tab, HEAD // 2, 1)
    low = lax.broadcasted_iota(jnp.int32, (T, HEAD), 1) < HEAD // 2
    cos_v[...] = jnp.where(low, tab, other)
    sin_v[...] = jnp.where(low, -other, tab)

    def project(slot):
        return jnp.dot(a_v[...], w_v[slot], preferred_element_type=F32).astype(BF16)

    def turned(t):
        t = t.astype(F32)
        return (t * cos_v[...] + pltpu.roll(t, HEAD // 2, 1) * sin_v[...]).astype(BF16)

    pl.semaphore_wait(barrier, 3)

    def keys_values(p, _):
        at = lax.rem(p, 2) * 2

        def ahead(w, n):
            @pl.when(p < PAIRS - 2)
            def _():
                weights(w, p + 2, at + n).start()

            @pl.when(p >= PAIRS - 2)
            def _():
                weights(wq, 2 * (p - (PAIRS - 2)) + n, at + n).start()

        weights(wk, p, at).wait()
        k = project(at)
        for i in range(2):
            k_s[me, 2 * p + i] = turned(k[:, i * HEAD : (i + 1) * HEAD])
        ahead(wk, 0)
        send(p, 0)
        weights(wv, p, at + 1).wait()
        v = project(at + 1)
        for i in range(2):
            v_s[me, 2 * p + i] = v[:, i * HEAD : (i + 1) * HEAD].T
        ahead(wv, 1)
        send(p, 1)

    lax.fori_loop(0, PAIRS, keys_values, None)

    out_weights(0).start()
    out_weights(1).start()

    blocks = HEADS // 2

    def queries(i, _):
        slot = lax.rem(i, 4)
        weights(wq, i, slot).wait()
        q = project(slot)
        for n in range(2):
            q_s[2 * i + n] = turned(q[:, n * HEAD : (n + 1) * HEAD])

        @pl.when(i + 4 < blocks)
        def _():
            weights(wq, i + 4, slot).start()

    lax.fori_loop(0, blocks, queries, None)

    strips = [(i, g) for i in range(2) for g in range(GROUP)]

    def with_ones(v):
        return jnp.concatenate([v, jnp.ones((8, v.shape[1]), BF16)], 0)

    def own(p):
        half = T // 2
        seen = lax.broadcasted_iota(jnp.int32, (half, half), 0) <= lax.broadcasted_iota(jnp.int32, (half, half), 1)
        scores = []
        for i, g in strips:
            k, q = k_s.at[me, 2 * p + i], q_s.at[2 * GROUP * p + GROUP * i + g]
            scores.append((_dot(k[:half], q[:half], 1, 1), _dot(k[...], q[half:], 1, 1)))
        weights = []
        for (i, g), (sa, sb) in zip(strips, scores):
            n = 2 * GROUP * p + GROUP * i + g
            sa = jnp.where(seen, sa, -jnp.inf)
            sb = jnp.concatenate([sb[:half], jnp.where(seen, sb[half:], -jnp.inf)], 0)
            ta, tb = sa.max(0, keepdims=True), sb.max(0, keepdims=True)
            top_s[n, :, :half] = ta
            top_s[n, :, half:] = tb
            weights.append((jnp.exp2((sa - ta) * E).astype(BF16), jnp.exp2((sb - tb) * E).astype(BF16)))
        for (i, g), (pa, pb) in zip(strips, weights):
            n = 2 * GROUP * p + GROUP * i + g
            v = with_ones(v_s[me, 2 * p + i])
            mix_s[n, :, :half] = _dot(v[:, :half], pa, 1, 0)
            mix_s[n, :, half:] = _dot(v, pb, 1, 0)

    def full(p, src):
        scores = [_dot(k_s[src, 2 * p + i], q_s[2 * GROUP * p + GROUP * i + g], 1, 1) for i, g in strips]
        weights, keeps = [], []
        for (i, g), s in zip(strips, scores):
            n = 2 * GROUP * p + GROUP * i + g
            old = top_s[n]
            top = jnp.maximum(old, s.max(0, keepdims=True))
            top_s[n] = top
            weights.append(jnp.exp2((s - top) * E).astype(BF16))
            keeps.append(jnp.exp2((old - top) * E))
        for (i, g), w, keep in zip(strips, weights, keeps):
            n = 2 * GROUP * p + GROUP * i + g
            mix_s[n] = mix_s[n] * keep + _dot(with_ones(v_s[src, 2 * p + i]), w, 1, 0)

    def local(p, _):
        own(p)

        @pl.when(lax.rem(me, 2) == 1)
        def _():
            for kv in range(2):
                move(me - 1, p, kv, near_sem.at[p, kv], me).wait_recv()
            full(p, me - 1)

    lax.fori_loop(0, PAIRS, local, None)

    def out_copy(c):
        cols = pl.ds(pl.multiple_of(c * CHUNK, CHUNK), CHUNK)
        return pltpu.make_async_copy(a_v.at[:, cols], out_hbm.at[:, cols], out_sem.at[c])

    def rest(p, _):
        @pl.when(me >= 2)
        def _():
            for src in range(2):
                for kv in range(2):
                    move(src, p, kv, hand_sem.at[src, p, kv], me).wait_recv()

                    @pl.when(me == 2)
                    def _():
                        hand(src, p, kv).start()

            lax.fori_loop(0, 2, lambda src, _: full(p, src), None)

        for i, g in strips:
            n = 2 * GROUP * p + GROUP * i + g
            at = (GROUP * i + g) * HEAD
            o_s[:, at : at + HEAD] = (mix_s[n, :HEAD] * (1 / mix_s[n, HEAD : HEAD + 1])).astype(BF16).T

        slot = lax.rem(p, 2)
        out_weights(p).wait()

        def columns(c, _):
            cols = pl.ds(pl.multiple_of(c * CHUNK, CHUNK), CHUNK)

            @pl.when(p == 0)
            def _():
                y_s[:, cols] = x_v[:, cols].astype(F32)

            y_s[:, cols] += jnp.dot(o_s[...], wo_v[slot, :, cols], preferred_element_type=F32)

            @pl.when(p == PAIRS - 1)
            def _():
                a_v[:, cols] = y_s[:, cols].astype(BF16)
                out_copy(c).start()

        lax.fori_loop(0, D // CHUNK, columns, None)

        @pl.when(p + 2 < PAIRS)
        def _():
            out_weights(p + 2).start()

    lax.fori_loop(0, PAIRS, rest, None)

    for p in range(PAIRS):
        for kv in range(2):
            @pl.when(me < 2)
            def _():
                link(p, kv).wait_send()

            @pl.when(lax.rem(me, 2) == 0)
            def _():
                near(p, kv).wait_send()

            @pl.when(me == 2)
            def _():
                for src in range(2):
                    hand(src, p, kv).wait_send()
    for c in range(D // CHUNK):
        out_copy(c).wait()


def solution(mesh):
    def step(x, gain, wq, wk, wv, wo):
        table = jnp.asarray(_table(T * mesh.shape["sp"]))
        anywhere = pl.BlockSpec(memory_space=pl.ANY)
        dma = pltpu.SemaphoreType.DMA
        return pl.pallas_call(
            _kernel,
            out_shape=jax.ShapeDtypeStruct((T, D), BF16),
            in_specs=[anywhere, pl.BlockSpec(memory_space=pltpu.VMEM)] + [anywhere] * 5,
            out_specs=anywhere,
            scratch_shapes=[
                pltpu.VMEM((T, D), BF16),
                pltpu.VMEM((T, D), BF16),
                pltpu.VMEM((T, HEAD), F32),
                pltpu.VMEM((T, HEAD), F32),
                pltpu.VMEM((T, HEAD), F32),
                pltpu.VMEM((4, D, 256), BF16),
                pltpu.VMEM((2, GROUP * 2 * HEAD, D), BF16),
                pltpu.VMEM((HEADS, T, HEAD), BF16),
                pltpu.VMEM((4, KV, T, HEAD), BF16),
                pltpu.VMEM((4, KV, HEAD, T), BF16),
                pltpu.VMEM((HEADS, 1, T), F32),
                pltpu.VMEM((HEADS, HEAD + 8, T), F32),
                pltpu.VMEM((T, GROUP * 2 * HEAD), BF16),
                pltpu.VMEM((T, D), F32),
                dma((4,)), dma, dma((4,)), dma((2,)), dma((D // CHUNK,)),
                dma((PAIRS, 2)), dma((PAIRS, 2)), dma((2, PAIRS, 2)), dma((4, PAIRS, 2)),
            ],
            compiler_params=pltpu.CompilerParams(collective_id=0, has_side_effects=True, vmem_limit_bytes=67043328),
            name="layer",
        )(x, gain.reshape(1, D), table, wq, wk, wv, wo)

    tokens, whole = P(("dp", "sp"), None), P(None, None)
    return jax.shard_map(
        step,
        mesh=mesh,
        in_specs=(tokens, P(None), whole, whole, whole, whole),
        out_specs=tokens,
        check_vma=False,
    )
```

```python
import functools

import jax
import jax.numpy as jnp
import numpy as np
from jax import lax
from jax.experimental import pallas as pl
from jax.experimental.pallas import tpu as pltpu
from jax.sharding import PartitionSpec as P

HEAD = 128
HEADS = 24
KV = 8
D = 3072
T = 512
THETA = 10000
LOG2E = 1.4426950408889634
E = HEAD**-0.5 * LOG2E
PAIRS = KV // 2
GROUP = HEADS // KV
CHUNK = 512
DEEP = 2 * GROUP * HEAD
SLOTS = 12
OUT = 2 * PAIRS + HEADS // 2
MESH = pl.DeviceIdType.MESH
F32, BF16 = jnp.float32, jnp.bfloat16


def _dot(a, b, ca, cb):
    return lax.dot_general(a, b, (((ca,), (cb,)), ((), ())), preferred_element_type=F32)


def _table(rows):
    half = HEAD // 2
    rate = np.float32(THETA) ** (-np.arange(half, dtype=np.float32) / np.float32(half))
    angle = (np.arange(rows, dtype=np.float32)[:, None] * rate.astype(np.float32)).astype(np.float64)
    return np.concatenate([np.cos(angle), np.sin(angle)], 1).astype(np.float32)


def _kernel(x_hbm, gain_ref, tab_hbm, wq, wk, wv, wo, out_hbm, x_v, a_v, tab_v, cos_v, sin_v, w_v, q_s, k_s, v_s, top_s, mix_s, o_s, y_s,
            x_sem, tab_sem, w_sem, out_sem, link_sem, near_sem, hand_sem, recv_sem):
    me = lax.axis_index("sp")

    rows = T // 4
    x_copies = [pltpu.make_async_copy(x_hbm.at[pl.ds(i * rows, rows)], x_v.at[pl.ds(i * rows, rows)], x_sem.at[i]) for i in range(4)]
    tab_copy = pltpu.make_async_copy(tab_hbm.at[pl.ds(pl.multiple_of(me * T, T), T)], tab_v, tab_sem)

    def weights(n):
        slot = n % SLOTS
        if n < 2 * PAIRS + HEADS // 2:
            w, i = ((wk, wv)[n % 2], n // 2) if n < 2 * PAIRS else (wq, n - 2 * PAIRS)
            return [pltpu.make_async_copy(w.at[:, i * 256 : (i + 1) * 256], w_v.at[slot], w_sem.at[slot])]
        p, c = divmod(n - OUT, 3)
        rows = pl.ds(p * DEEP, DEEP)
        return [
            pltpu.make_async_copy(wo.at[rows, pl.ds((4 * c + r) * 256, 256)], w_v.at[slot, pl.ds(r * DEEP, DEEP)], w_sem.at[slot])
            for r in range(4)
        ]

    def fetch(blocks):
        for n in blocks:
            for c in weights(n):
                c.start()

    def arrive(blocks):
        for n in blocks:
            pltpu.make_async_copy(wq.at[:, :256], w_v.at[n % SLOTS], w_sem.at[n % SLOTS]).wait()

    for c in x_copies:
        c.start()
    fetch(range(2))
    tab_copy.start()
    fetch(range(2, SLOTS))

    barrier = pltpu.get_barrier_semaphore()
    for i in range(1, 4):
        pl.semaphore_signal(barrier, inc=1, device_id={"sp": lax.rem(me + i, 4)}, device_id_type=MESH)

    def move(src, p, kv, send, to):
        buf = (k_s, v_s)[kv]
        part = buf.at[src, pl.ds(2 * p, 2)]
        return pltpu.make_async_remote_copy(part, part, send_sem=send, recv_sem=recv_sem.at[src, p, kv], device_id={"sp": to}, device_id_type=MESH)

    def link(p, kv):
        return move(me, p, kv, link_sem.at[p, kv], 2)

    def near(p, kv):
        return move(me, p, kv, near_sem.at[p, kv], lax.rem(me + 1, 4))

    def hand(src, p, kv):
        return move(src, p, kv, hand_sem.at[src, p, kv], 3)

    def send(p, kv):
        @pl.when(me < 2)
        def _():
            link(p, kv).start()

        @pl.when(lax.rem(me, 2) == 0)
        def _():
            near(p, kv).start()

    for i, c in enumerate(x_copies):
        c.wait()
        here = pl.ds(i * rows, rows)
        total = jnp.zeros((rows, 128), F32)
        for at in range(0, D, 128):
            t = x_v[here, at : at + 128].astype(F32)
            total += t * t
        scale = lax.rsqrt(jnp.sum(total, 1, keepdims=True) * (1 / D) + 1e-6)
        for at in range(0, D, 128):
            t = x_v[here, at : at + 128].astype(F32)
            y_s[here, at : at + 128] = t
            a_v[here, at : at + 128] = (t * scale * gain_ref[at : at + 128].astype(F32)).astype(BF16)

    tab_copy.wait()
    tab = tab_v[...]
    other = pltpu.roll(tab, HEAD // 2, 1)
    low = lax.broadcasted_iota(jnp.int32, (T, HEAD), 1) < HEAD // 2
    cos_v[...] = jnp.where(low, tab, other)
    sin_v[...] = jnp.where(low, -other, tab)

    def project(slot):
        return jnp.dot(a_v[...], w_v[slot], preferred_element_type=F32).astype(BF16)

    def turned(t):
        t = t.astype(F32)
        return (t * cos_v[...] + pltpu.roll(t, HEAD // 2, 1) * sin_v[...]).astype(BF16)

    pl.semaphore_wait(barrier, 3)

    def keys_values(pairs):
        blocks = range(2 * pairs[0], 2 * pairs[-1] + 2)
        arrive(blocks)
        for n in blocks:
            t = project(n % SLOTS)
            for i in range(2):
                head = t[:, i * HEAD : (i + 1) * HEAD]
                if n % 2 == 0:
                    k_s[me, n + i] = turned(head)
                else:
                    v_s[me, n - 1 + i] = head.T
        for p in pairs:
            send(p, 0)
            send(p, 1)
        fetch(n + SLOTS for n in blocks)

    keys_values(range(1))
    keys_values(range(1, PAIRS))

    for first in range(0, HEADS // 2, 4):
        blocks = range(2 * PAIRS + first, 2 * PAIRS + first + 4)
        arrive(blocks)
        for i in range(4):
            q = project(blocks[i] % SLOTS)
            for n in range(2):
                q_s[2 * (first + i) + n] = turned(q[:, n * HEAD : (n + 1) * HEAD])
        fetch(n + SLOTS for n in blocks)

    strips = [(i, g) for i in range(2) for g in range(GROUP)]

    def with_ones(v):
        return jnp.concatenate([v, jnp.ones((8, v.shape[1]), BF16)], 0)

    def own(p):
        half = T // 2
        seen = lax.broadcasted_iota(jnp.int32, (half, half), 0) <= lax.broadcasted_iota(jnp.int32, (half, half), 1)
        scores = []
        for i, g in strips:
            k, q = k_s.at[me, 2 * p + i], q_s.at[2 * GROUP * p + GROUP * i + g]
            scores.append((_dot(k[:half], q[:half], 1, 1), _dot(k[...], q[half:], 1, 1)))
        weights = []
        for (i, g), (sa, sb) in zip(strips, scores):
            n = 2 * GROUP * p + GROUP * i + g
            sa = jnp.where(seen, sa, -jnp.inf)
            sb = jnp.concatenate([sb[:half], jnp.where(seen, sb[half:], -jnp.inf)], 0)
            ta, tb = sa.max(0, keepdims=True), sb.max(0, keepdims=True)
            top_s[n, :, :half] = ta
            top_s[n, :, half:] = tb
            weights.append((jnp.exp2((sa - ta) * E).astype(BF16), jnp.exp2((sb - tb) * E).astype(BF16)))
        for (i, g), (pa, pb) in zip(strips, weights):
            n = 2 * GROUP * p + GROUP * i + g
            v = with_ones(v_s[me, 2 * p + i])
            mix_s[n, :, :half] = _dot(v[:, :half], pa, 1, 0)
            mix_s[n, :, half:] = _dot(v, pb, 1, 0)

    def full(p, src):
        scores = [_dot(k_s[src, 2 * p + i], q_s[2 * GROUP * p + GROUP * i + g], 1, 1) for i, g in strips]
        weights, keeps = [], []
        for (i, g), s in zip(strips, scores):
            n = 2 * GROUP * p + GROUP * i + g
            old = top_s[n]
            top = jnp.maximum(old, s.max(0, keepdims=True))
            top_s[n] = top
            weights.append(jnp.exp2((s - top) * E).astype(BF16))
            keeps.append(jnp.exp2((old - top) * E))
        for (i, g), w, keep in zip(strips, weights, keeps):
            n = 2 * GROUP * p + GROUP * i + g
            mix_s[n] = mix_s[n] * keep + _dot(with_ones(v_s[src, 2 * p + i]), w, 1, 0)

    def local(p, _):
        own(p)

        @pl.when(lax.rem(me, 2) == 1)
        def _():
            for kv in range(2):
                move(me - 1, p, kv, near_sem.at[p, kv], me).wait_recv()
            full(p, me - 1)

    lax.fori_loop(0, PAIRS, local, None)

    def out_copy(c):
        cols = pl.ds(c * CHUNK, CHUNK)
        return pltpu.make_async_copy(a_v.at[:, cols], out_hbm.at[:, cols], out_sem.at[c])

    def rest(p, last):
        @pl.when(me >= 2)
        def _():
            for src in range(2):
                for kv in range(2):
                    move(src, p, kv, hand_sem.at[src, p, kv], me).wait_recv()

                    @pl.when(me == 2)
                    def _():
                        hand(src, p, kv).start()

            lax.fori_loop(0, 2, lambda src, _: full(p, src), None)

        for i, g in strips:
            n = 2 * GROUP * p + GROUP * i + g
            at = (GROUP * i + g) * HEAD
            o_s[:, at : at + HEAD] = (mix_s[n, :HEAD] * (1 / mix_s[n, HEAD : HEAD + 1])).astype(BF16).T

        for c in range(D // CHUNK):
            for half in range(2):
                m = 2 * c + half
                cols = slice(m * 256, (m + 1) * 256)
                slot = (OUT + 3 * p + m // 4) % SLOTS if last else lax.rem(OUT + 3 * p + m // 4, SLOTS)
                y = y_s[:, cols] + jnp.dot(o_s[...], w_v[slot, m % 4 * DEEP : (m % 4 + 1) * DEEP, :], preferred_element_type=F32)
                if last:
                    a_v[:, cols] = y.astype(BF16)
                else:
                    y_s[:, cols] = y
            if last:
                out_copy(c).start()

    arrive(range(OUT, OUT + SLOTS))
    lax.fori_loop(0, PAIRS - 1, lambda p, _: rest(p, False), None)
    rest(PAIRS - 1, True)

    for p in range(PAIRS):
        for kv in range(2):
            @pl.when(me < 2)
            def _():
                link(p, kv).wait_send()

            @pl.when(lax.rem(me, 2) == 0)
            def _():
                near(p, kv).wait_send()

            @pl.when(me == 2)
            def _():
                for src in range(2):
                    hand(src, p, kv).wait_send()
    for c in range(D // CHUNK):
        out_copy(c).wait()


def solution(mesh):
    def step(x, gain, wq, wk, wv, wo):
        table = jnp.asarray(_table(T * mesh.shape["sp"]))
        anywhere = pl.BlockSpec(memory_space=pl.ANY)
        dma = pltpu.SemaphoreType.DMA
        return pl.pallas_call(
            _kernel,
            out_shape=jax.ShapeDtypeStruct((T, D), BF16),
            in_specs=[anywhere, pl.BlockSpec(memory_space=pltpu.VMEM)] + [anywhere] * 5,
            out_specs=anywhere,
            scratch_shapes=[
                pltpu.VMEM((T, D), BF16),
                pltpu.VMEM((T, D), BF16),
                pltpu.VMEM((T, HEAD), F32),
                pltpu.VMEM((T, HEAD), F32),
                pltpu.VMEM((T, HEAD), F32),
                pltpu.VMEM((SLOTS, D, 256), BF16),
                pltpu.VMEM((HEADS, T, HEAD), BF16),
                pltpu.VMEM((4, KV, T, HEAD), BF16),
                pltpu.VMEM((4, KV, HEAD, T), BF16),
                pltpu.VMEM((HEADS, 1, T), F32),
                pltpu.VMEM((HEADS, HEAD + 8, T), F32),
                pltpu.VMEM((T, DEEP), BF16),
                pltpu.VMEM((T, D), F32),
                dma((4,)), dma, dma((SLOTS,)), dma((D // CHUNK,)),
                dma((PAIRS, 2)), dma((PAIRS, 2)), dma((2, PAIRS, 2)), dma((4, PAIRS, 2)),
            ],
            compiler_params=pltpu.CompilerParams(collective_id=0, has_side_effects=True, vmem_limit_bytes=67043328),
            name="layer",
        )(x, gain, table, wq, wk, wv, wo)

    tokens, whole = P(("dp", "sp"), None), P(None, None)
    return jax.shard_map(
        step,
        mesh=mesh,
        in_specs=(tokens, P(None), whole, whole, whole, whole),
        out_specs=tokens,
        check_vma=False,
    )
```

```python
import functools

import jax
import jax.numpy as jnp
import numpy as np
from jax import lax
from jax.experimental import pallas as pl
from jax.experimental.pallas import tpu as pltpu
from jax.sharding import PartitionSpec as P

HEAD = 128
HEADS = 24
KV = 8
D = 3072
T = 512
THETA = 10000
LOG2E = 1.4426950408889634
E = HEAD**-0.5 * LOG2E
NEG = -1e30
PAIRS = KV // 2
GROUP = HEADS // KV
CHUNK = 512
DEEP = 2 * GROUP * HEAD
SLOTS = 12
QS = 2 * PAIRS
OUT = QS + HEADS // 2
MESH = pl.DeviceIdType.MESH
F32, BF16 = jnp.float32, jnp.bfloat16


def _dot(a, b, ca, cb):
    return lax.dot_general(a, b, (((ca,), (cb,)), ((), ())), preferred_element_type=F32)


def _table(places):
    half = HEAD // 2
    rate = (np.float32(THETA) ** (-np.arange(half, dtype=np.float32) / np.float32(half))).astype(np.float64)
    angle = np.asarray(places, np.float64)[:, None] * rate
    return np.concatenate([np.cos(angle), np.sin(angle)], 1).astype(np.float32)


def _kernel(x_hbm, gain_hbm, start_hbm, tab_hbm, wq, wk, wv, wo, out_hbm, x_v, a_v, gain_v, start_v, tab_v, turn_v, w_v, q_s, k_s, v_s, top_s, mix_s, o_s, y_s,
            x_sem, small_sem, w_sem, out_sem, link_sem, near_sem, hand_sem, recv_sem, lend_sem, lent_sem,
            give_sem, given_sem):
    me = lax.axis_index("sp")

    rows = T // 4
    x_copies = [pltpu.make_async_copy(x_hbm.at[pl.ds(i * rows, rows)], x_v.at[pl.ds(i * rows, rows)], x_sem.at[i]) for i in range(4)]

    def columns(i):
        return pl.ds(i * 256 if isinstance(i, int) else pl.multiple_of(i * 256, 256), 256)

    def weights(w, i, n):
        slot = n % SLOTS
        return pltpu.make_async_copy(w.at[:, columns(i)], w_v.at[slot], w_sem.at[slot])

    def fetch_out(p):
        for c in range(3):
            slot = (OUT + 3 * p + c) % SLOTS
            for r in range(4):
                rows = pl.ds(p * DEEP if isinstance(p, int) else pl.multiple_of(p * DEEP, DEEP), DEEP)
                pltpu.make_async_copy(wo.at[rows, columns(4 * c + r)], w_v.at[slot, pl.ds(r * DEEP, DEEP)], w_sem.at[slot]).start()

    def arrive(n):
        pltpu.make_async_copy(wq.at[:, :256], w_v.at[n % SLOTS], w_sem.at[n % SLOTS]).wait()

    gain_copy = pltpu.make_async_copy(gain_hbm, gain_v, small_sem.at[0])
    angle_copies = [
        pltpu.make_async_copy(start_hbm.at[pl.ds(me * 8, 8)], start_v, small_sem.at[1]),
        pltpu.make_async_copy(tab_hbm, tab_v, small_sem.at[2]),
    ]
    gain_copy.start()
    for c in x_copies:
        c.start()
    weights(wk, 0, 0).start()
    weights(wv, 0, 1).start()
    for c in angle_copies:
        c.start()

    barrier = pltpu.get_barrier_semaphore()
    for i in range(1, 4):
        pl.semaphore_signal(barrier, inc=1, device_id={"sp": lax.rem(me + i, 4)}, device_id_type=MESH)

    def move(src, p, kv, send, to):
        buf = (k_s, v_s)[kv]
        part = buf.at[src, pl.ds(2 * p, 2)]
        return pltpu.make_async_remote_copy(part, part, send_sem=send, recv_sem=recv_sem.at[src, p, kv], device_id={"sp": to}, device_id_type=MESH)

    def link(p, kv):
        return move(me, p, kv, link_sem.at[p, kv], 2)

    def near(p, kv):
        return move(me, p, kv, near_sem.at[p, kv], lax.rem(me + 1, 4))

    def hand(src, p, kv):
        return move(src, p, kv, hand_sem.at[src, p, kv], 3)

    odd, even = lax.rem(me, 2) == 1, lax.rem(me, 2) == 0

    def lend(j, to):
        queries = pl.ds(2 * GROUP * (2 + j), 2 * GROUP), pl.ds(HEADS + 2 * GROUP * j, 2 * GROUP)
        return pltpu.make_async_remote_copy(
            q_s.at[queries[0]], q_s.at[queries[1]], lend_sem.at[j], lent_sem.at[j], device_id={"sp": to}, device_id_type=MESH
        )

    def give(j, to):
        part = pl.ds(HEADS + 2 * GROUP * j, 2 * GROUP)
        return [
            pltpu.make_async_remote_copy(
                buf.at[part], buf.at[part], give_sem.at[j, i], given_sem.at[j, i], device_id={"sp": to}, device_id_type=MESH
            )
            for i, buf in enumerate((mix_s, top_s))
        ]

    def send(p, kv):
        @pl.when(me < 2)
        def _():
            link(p, kv).start()

        if p < 2:

            @pl.when(even)
            def _():
                near(p, kv).start()

    with jax.named_scope("norm"):
        gain_copy.wait()
        for i, c in enumerate(x_copies):
            c.wait()
            here = pl.ds(i * rows, rows)
            total = jnp.zeros((rows, 128), F32)
            for at in range(0, D, 128):
                t = x_v[here, at : at + 128].astype(F32)
                total += t * t
            scale = lax.rsqrt(jnp.sum(total, 1, keepdims=True) * (1 / D) + 1e-6)
            for at in range(0, D, 128):
                t = x_v[here, at : at + 128].astype(F32)
                y_s[here, at : at + 128] = t
                a_v[here, at : at + 128] = (t * scale * gain_v[at : at + 128].astype(F32)).astype(BF16)

        for n in range(2, 2 * PAIRS):
            weights((wk, wv)[n % 2], n // 2, n).start()
        for i in range(SLOTS - 2 * PAIRS):
            weights(wq, i, QS + i).start()

    def project(n):
        return jnp.dot(a_v[...], w_v[n % SLOTS], preferred_element_type=F32).astype(BF16)

    def turned(t, at):
        t = t.astype(F32)
        return (t * turn_v[at] + pltpu.roll(t, HEAD // 2, 1) * turn_v[at + 1]).astype(BF16)

    with jax.named_scope("barrier"):
        pl.semaphore_wait(barrier, 3)

    def make_angles():
        low = lax.broadcasted_iota(jnp.int32, (T, HEAD), 1) < HEAD // 2

        def halves(tab):
            other, first = pltpu.roll(tab, HEAD // 2, 1), low[: tab.shape[0]]
            return jnp.where(first, tab, other), jnp.where(first, other, tab)

        (ca, sa), (cb, sb) = halves(start_v[...]), halves(tab_v[...])
        ca, sa = ca[:1], sa[:1]
        cos, sin = ca * cb - sa * sb, sa * cb + ca * sb
        sin = jnp.where(low, -sin, sin)
        for i, t in enumerate((cos, sin, cos * E, sin * E)):
            turn_v[i] = t

    def keys_values(pairs):
        blocks = range(2 * pairs[0], 2 * pairs[-1] + 2)
        for n in blocks:
            arrive(n)
        if pairs[0] == 0:
            for c in angle_copies:
                c.wait()
        for n in blocks:
            t = project(n)
            if n == 0:
                make_angles()
            for i in range(2):
                head = t[:, i * HEAD : (i + 1) * HEAD]
                if n % 2 == 0:
                    k_s[me, n + i] = turned(head, 0)
                else:
                    v_s[me, n - 1 + i] = head.T
        for p in pairs:
            send(p, 0)
            send(p, 1)
        for n in blocks:
            weights(wq, n + SLOTS - QS, n + SLOTS).start()

    with jax.named_scope("keys_values_first"):
        keys_values(range(1))
    with jax.named_scope("keys_values"):
        keys_values(range(1, PAIRS))

    def query_jobs(p):
        def job(c):
            i = 3 * p + c
            q = project((QS + i) % SLOTS)
            for n in range(2):
                q_s[2 * i + n] = turned(q[:, n * HEAD : (n + 1) * HEAD], 2)

        return [functools.partial(job, c) for c in range(3)]

    def out_copy(c):
        cols = pl.ds(c * CHUNK, CHUNK)
        return pltpu.make_async_copy(a_v.at[:, cols], out_hbm.at[:, cols], out_sem.at[c])

    def out_jobs(p, last=False):
        def job(m):
            cols = slice(m * 256, (m + 1) * 256)
            slot = (OUT + 3 * p + m // 4) % SLOTS
            y = y_s[:, cols] + jnp.dot(o_s[...], w_v[slot, m % 4 * DEEP : (m % 4 + 1) * DEEP, :], preferred_element_type=F32)
            if last:
                a_v[:, cols] = y.astype(BF16)
                if m % 2 == 1:
                    out_copy(m // 2).start()
            else:
                y_s[:, cols] = y

        return [functools.partial(job, m) for m in range(12)]

    strips = [(i, g) for i in range(2) for g in range(GROUP)]
    half = T // 2

    def row(p, i, g):
        return 2 * GROUP * p + GROUP * i + g

    def with_ones(v):
        return jnp.concatenate([v, jnp.ones((8, v.shape[1]), BF16)], 0)

    def staged(stages, jobs=()):
        scores, weigh, mix = stages
        count, done, s, w = len(strips), 0, {}, {}
        for at in range(count + 2):
            if at < count:
                s[at] = scores(*strips[at])
            upto = len(jobs) * (at + 1) // (count + 2)
            for job in jobs[done:upto]:
                job()
            done = upto
            if 0 <= at - 1 < count:
                w[at - 1] = weigh(*strips[at - 1], s.pop(at - 1))
            if 0 <= at - 2 < count:
                mix(*strips[at - 2], w.pop(at - 2))

    def own(p):
        seen = lax.broadcasted_iota(jnp.int32, (half, half), 0) <= lax.broadcasted_iota(jnp.int32, (half, half), 1)

        def scores(i, g):
            k, q = k_s.at[me, 2 * p + i], q_s.at[row(p, i, g)]
            return _dot(k[:half], q[:half], 1, 1), _dot(k[...], q[half:], 1, 1)

        def weigh(i, g, s):
            n, (sa, sb) = row(p, i, g), s
            sa = jnp.where(seen, sa, -jnp.inf)
            sb = jnp.concatenate([sb[:half], jnp.where(seen, sb[half:], -jnp.inf)], 0)
            ta, tb = sa.max(0, keepdims=True), sb.max(0, keepdims=True)
            top_s[n, :, :half] = ta
            top_s[n, :, half:] = tb
            return jnp.exp2(sa - ta).astype(BF16), jnp.exp2(sb - tb).astype(BF16)

        def mix(i, g, w):
            n, (wa, wb), v = row(p, i, g), w, with_ones(v_s[me, 2 * p + i])
            mix_s[n, :, :half] = _dot(v[:, :half], wa, 1, 0)
            mix_s[n, :, half:] = _dot(v, wb, 1, 0)

        return scores, weigh, mix

    def full(p, base, srcs):
        def scores(i, g):
            return [_dot(k_s[src, 2 * p + i], q_s[base + GROUP * i + g], 1, 1) for src in srcs]

        def weigh(i, g, s):
            n = base + GROUP * i + g
            old = top = top_s[n]
            for part in s:
                top = jnp.maximum(top, part.max(0, keepdims=True))
            top_s[n] = top
            return [jnp.exp2(part - top).astype(BF16) for part in s], jnp.exp2(old - top)

        def mix(i, g, w):
            n, (parts, keep) = base + GROUP * i + g, w
            mix_s[n] = mix_s[n] * keep + sum(_dot(with_ones(v_s[src, 2 * p + i]), part, 1, 0) for src, part in zip(srcs, parts))

        return scores, weigh, mix

    def merge(p):
        for i in range(2 * GROUP):
            a, b = row(p, 0, 0) + i, HEADS + row(p - 2, 0, 0) + i
            top = jnp.maximum(top_s[a], top_s[b])
            mix_s[a] = mix_s[a] * jnp.exp2(top_s[a] - top) + mix_s[b] * jnp.exp2(top_s[b] - top)
            top_s[a] = top

    def finish(p):
        for i, g in strips:
            n, at = row(p, i, g), (GROUP * i + g) * HEAD
            o_s[:, at : at + HEAD] = (mix_s[n, :HEAD] * (1 / mix_s[n, HEAD : HEAD + 1])).astype(BF16).T

    def arrive_queries(p):
        for c in range(3):
            arrive(QS + 3 * p + c)

    with jax.named_scope("queries"):
        arrive_queries(0)
        for job in query_jobs(0):
            job()
        fetch_out(0)

    def take(p):
        for src in range(2):
            for kv in range(2):
                move(src, p, kv, hand_sem.at[src, p, kv], me).wait_recv()

                @pl.when(me == 2)
                def _():
                    hand(src, p, kv).start()

    def local(p, _):
        with jax.named_scope("own_queries"):
            arrive_queries(p + 1)
            staged(own(p), query_jobs(p + 1))
            fetch_out(p + 1)

        @pl.when(odd & (p >= 1))
        def _():
            lend(p - 1, me - 1).start()

    lax.fori_loop(0, PAIRS - 1, local, None)
    @pl.when(me == 2)
    def _():
        take(0)

    with jax.named_scope("own"):
        staged(own(PAIRS - 1))

    def neighbour(j, _):
        @pl.when(odd)
        def _():
            for kv in range(2):
                move(me - 1, j, kv, near_sem.at[j, kv], me).wait_recv()

        @pl.when(even)
        def _():
            lend(j, me).wait_recv()

            @pl.when((me == 2) & (j == 1))
            def _():
                take(1)

            for i in range(2 * GROUP):
                n = HEADS + 2 * GROUP * j + i
                top_s[n] = jnp.full((1, T), NEG, F32)
                mix_s[n] = jnp.zeros((HEAD + 8, T), F32)

        with jax.named_scope("neighbour"):
            base = 2 * GROUP * j + jnp.where(odd, 0, HEADS)
            staged(full(j + jnp.where(odd, 0, 2), base, (me - lax.rem(me, 2),)))

        @pl.when(even)
        def _():
            for c in give(j, me + 1):
                c.start()

    lax.fori_loop(0, 2, neighbour, None)

    for n in range(OUT, OUT + SLOTS):
        arrive(n)

    def remote(p, _):
        @pl.when(odd & (p >= 2))
        def _():
            with jax.named_scope("merge"):
                for c in give(p - 2, me):
                    c.wait_recv()
                merge(p)

        @pl.when(me >= 2)
        def _():
            with jax.named_scope("linked_wait"):

                @pl.when((me == 3) | (p == PAIRS - 1))
                def _():
                    take(p)

            with jax.named_scope("linked"):
                staged(full(p, row(p, 0, 0), (0, 1)))

        @pl.when((me == 2) & (p == 1))
        def _():
            take(2)

        with jax.named_scope("finish"):
            finish(p)

        @pl.when(p < PAIRS - 1)
        def _():
            with jax.named_scope("out"):
                for job in out_jobs(p):
                    job()

    lax.fori_loop(0, PAIRS, remote, None)
    with jax.named_scope("last_out"):
        for job in out_jobs(PAIRS - 1, True):
            job()

    for p in range(PAIRS):
        for kv in range(2):
            @pl.when(me < 2)
            def _():
                link(p, kv).wait_send()

            @pl.when(me == 2)
            def _():
                for src in range(2):
                    hand(src, p, kv).wait_send()

    for j in range(2):
        @pl.when(odd)
        def _():
            lend(j, me - 1).wait_send()

        @pl.when(even)
        def _():
            for c in [near(j, 0), near(j, 1)] + give(j, me + 1):
                c.wait_send()

    for c in range(D // CHUNK):
        out_copy(c).wait()


def solution(mesh):
    def step(x, gain, wq, wk, wv, wo):
        start = jnp.asarray(_table(np.repeat(np.arange(mesh.shape["sp"]) * T, 8)))
        table = jnp.asarray(_table(np.arange(T)))
        anywhere = pl.BlockSpec(memory_space=pl.ANY)
        dma = pltpu.SemaphoreType.DMA
        return pl.pallas_call(
            _kernel,
            out_shape=jax.ShapeDtypeStruct((T, D), BF16),
            in_specs=[anywhere] * 8,
            out_specs=anywhere,
            scratch_shapes=[
                pltpu.VMEM((T, D), BF16),
                pltpu.VMEM((T, D), BF16),
                pltpu.VMEM((D,), BF16),
                pltpu.VMEM((8, HEAD), F32),
                pltpu.VMEM((T, HEAD), F32),
                pltpu.VMEM((4, T, HEAD), F32),
                pltpu.VMEM((SLOTS, D, 256), BF16),
                pltpu.VMEM((HEADS + 4 * GROUP, T, HEAD), BF16),
                pltpu.VMEM((4, KV, T, HEAD), BF16),
                pltpu.VMEM((4, KV, HEAD, T), BF16),
                pltpu.VMEM((HEADS + 4 * GROUP, 1, T), F32),
                pltpu.VMEM((HEADS + 4 * GROUP, HEAD + 8, T), F32),
                pltpu.VMEM((T, DEEP), BF16),
                pltpu.VMEM((T, D), F32),
                dma((4,)), dma((3,)), dma((SLOTS,)), dma((D // CHUNK,)),
                dma((PAIRS, 2)), dma((2, 2)), dma((2, PAIRS, 2)), dma((4, PAIRS, 2)),
                dma((2,)), dma((2,)), dma((2, 2)), dma((2, 2)),
            ],
            compiler_params=pltpu.CompilerParams(collective_id=0, has_side_effects=True, vmem_limit_bytes=67043328),
            name="layer",
        )(x, gain, start, table, wq, wk, wv, wo)

    tokens, whole = P(("dp", "sp"), None), P(None, None)
    return jax.shard_map(
        step,
        mesh=mesh,
        in_specs=(tokens, P(None), whole, whole, whole, whole),
        out_specs=tokens,
        check_vma=False,
    )
```

```python
import functools

import jax
import jax.numpy as jnp
import numpy as np
from jax import lax
from jax.experimental import pallas as pl
from jax.experimental.pallas import tpu as pltpu
from jax.sharding import PartitionSpec as P

HEAD = 128
HEADS = 24
KV = 8
D = 3072
T = 512
THETA = 10000
LOG2E = 1.4426950408889634
E = HEAD**-0.5 * LOG2E
NEG = -1e30
PAIRS = KV // 2
GROUP = HEADS // KV
DEEP = 2 * GROUP * HEAD
SLOTS = 12
LIMIT = 67043328 - T * D * 2
MESH = pl.DeviceIdType.MESH
F32, BF16 = jnp.float32, jnp.bfloat16


def _dot(a, b, ca, cb):
    return lax.dot_general(a, b, (((ca,), (cb,)), ((), ())), preferred_element_type=F32)


def _table(places):
    half = HEAD // 2
    rate = (np.float32(THETA) ** (-np.arange(half, dtype=np.float32) / np.float32(half))).astype(np.float64)
    angle = np.asarray(places, np.float64)[:, None] * rate
    return np.concatenate([np.cos(angle), np.sin(angle)], 1).astype(np.float32)


def _kernel(x_hbm, gain_hbm, start_hbm, tab_hbm, wq, wk, wv, wo, out_v, a_v, gain_v, start_v, tab_v, turn_v, w_v, q_s, k_s, v_s, top_s, mix_s, o_s, y_s,
            x_sem, small_sem, w_sem, link_sem, near_sem, hand_sem, recv_sem, lend_sem, lent_sem,
            give_sem, given_sem):
    me = lax.axis_index("sp")

    rows = T // 4
    x_copies = [pltpu.make_async_copy(x_hbm.at[pl.ds(i * rows, rows)], a_v.at[pl.ds(i * rows, rows)], x_sem.at[i]) for i in range(4)]

    def columns(i):
        return pl.ds(i * 256 if isinstance(i, int) else pl.multiple_of(i * 256, 256), 256)

    def weights(w, i, slot):
        return pltpu.make_async_copy(w.at[:, columns(i)], w_v.at[slot], w_sem.at[slot])

    def place(p):
        return (3 * (p - 1) if p else 9) if isinstance(p, int) else jnp.where(p == 0, 9, 3 * (p - 1))

    def fetch_queries(p, cs):
        for c in cs:
            weights(wq, 3 * p + c, place(p) + c).start()

    def fetch_out(p):
        for c in range(3):
            slot = place(p) + c
            for r in range(4):
                rows = pl.ds(p * DEEP if isinstance(p, int) else pl.multiple_of(p * DEEP, DEEP), DEEP)
                pltpu.make_async_copy(wo.at[rows, columns(4 * c + r)], w_v.at[slot, pl.ds(r * DEEP, DEEP)], w_sem.at[slot]).start()

    def arrive(slot):
        weights(wq, 0, slot).wait()

    gain_copy = pltpu.make_async_copy(gain_hbm, gain_v, small_sem.at[0])
    angle_copies = [
        pltpu.make_async_copy(start_hbm.at[pl.ds(me * 8, 8)], start_v, small_sem.at[1]),
        pltpu.make_async_copy(tab_hbm, tab_v, small_sem.at[2]),
    ]
    gain_copy.start()
    for c in x_copies:
        c.start()
    weights(wk, 0, 0).start()
    weights(wv, 0, 1).start()
    for c in angle_copies:
        c.start()

    barrier = pltpu.get_barrier_semaphore()
    for i in range(1, 4):
        pl.semaphore_signal(barrier, inc=1, device_id={"sp": lax.rem(me + i, 4)}, device_id_type=MESH)

    def move(src, h, kv, send, to):
        part = (k_s, v_s)[kv].at[src, h]
        return pltpu.make_async_remote_copy(part, part, send_sem=send, recv_sem=recv_sem.at[src, h, kv], device_id={"sp": to}, device_id_type=MESH)

    def link(h, kv):
        return move(me, h, kv, link_sem.at[kv], 2)

    def near(h, kv):
        return move(me, h, kv, near_sem.at[kv], lax.rem(me + 1, 4))

    def hand(src, h, kv):
        return move(src, h, kv, hand_sem.at[kv], 3)

    odd, even = lax.rem(me, 2) == 1, lax.rem(me, 2) == 0

    def lend(j, to):
        queries = pl.ds(2 * GROUP * (2 + j), 2 * GROUP), pl.ds(HEADS + 2 * GROUP * j, 2 * GROUP)
        return pltpu.make_async_remote_copy(
            q_s.at[queries[0]], q_s.at[queries[1]], lend_sem, lent_sem.at[j], device_id={"sp": to}, device_id_type=MESH
        )

    def give(j, to):
        part = pl.ds(HEADS + 2 * GROUP * j, 2 * GROUP)
        return [
            pltpu.make_async_remote_copy(
                buf.at[part], buf.at[part], give_sem.at[i], given_sem.at[j, i], device_id={"sp": to}, device_id_type=MESH
            )
            for i, buf in enumerate((mix_s, top_s))
        ]

    def send(p, kvs):
        @pl.when(me < 2)
        def _():
            for i in range(2):
                for kv in kvs:
                    link(2 * p + i, kv).start()

        if p < 2:

            @pl.when(even)
            def _():
                for i in range(2):
                    for kv in kvs:
                        near(2 * p + i, kv).start()

    with jax.named_scope("norm"):
        gain_copy.wait()
        for i, c in enumerate(x_copies):
            c.wait()
            here = pl.ds(i * rows, rows)
            total = jnp.zeros((rows, 128), F32)
            for at in range(0, D, 128):
                t = a_v[here, at : at + 128].astype(F32)
                total += t * t
            scale = lax.rsqrt(jnp.sum(total, 1, keepdims=True) * (1 / D) + 1e-6)
            for at in range(0, D, 128):
                t = a_v[here, at : at + 128].astype(F32)
                y_s[here, at : at + 128] = t
                a_v[here, at : at + 128] = (t * scale * gain_v[at : at + 128].astype(F32)).astype(BF16)

        for n in range(2, 2 * PAIRS):
            weights((wk, wv)[n % 2], n // 2, n + 1).start()
        fetch_queries(0, range(3))
        fetch_queries(1, [2])

    def project(slot):
        return jnp.dot(a_v[...], w_v[slot], preferred_element_type=F32).astype(BF16)

    def turned(t, at):
        t = t.astype(F32)
        return (t * turn_v[at] + pltpu.roll(t, HEAD // 2, 1) * turn_v[at + 1]).astype(BF16)

    with jax.named_scope("barrier"):
        pl.semaphore_wait(barrier, 3)

    def make_angles():
        low = lax.broadcasted_iota(jnp.int32, (T, HEAD), 1) < HEAD // 2

        def halves(tab):
            other, first = pltpu.roll(tab, HEAD // 2, 1), low[: tab.shape[0]]
            return jnp.where(first, tab, other), jnp.where(first, other, tab)

        (ca, sa), (cb, sb) = halves(start_v[...]), halves(tab_v[...])
        ca, sa = ca[:1], sa[:1]
        cos, sin = ca * cb - sa * sb, sa * cb + ca * sb
        sin = jnp.where(low, -sin, sin)
        for i, t in enumerate((cos, sin, cos * E, sin * E)):
            turn_v[i] = t

    def keys_values(blocks):
        for n in blocks:
            t = project(n if n < 2 else n + 1)
            if n == 0:
                make_angles()
            for i in range(2):
                head = t[:, i * HEAD : (i + 1) * HEAD]
                if n % 2 == 0:
                    k_s[me, n + i] = turned(head, 0)
                else:
                    v_s[me, n - 1 + i] = head.T

    with jax.named_scope("first_keys"):
        for c in angle_copies:
            c.wait()
        arrive(0)
        keys_values([0])
        send(0, [0])
    with jax.named_scope("first_values"):
        arrive(1)
        keys_values([1])
        send(0, [1])
        fetch_queries(1, [0, 1])

    def query_jobs(p):
        def job(c):
            i = 3 * p + c
            q = project(place(p) + c)
            for n in range(2):
                q_s[2 * i + n] = turned(q[:, n * HEAD : (n + 1) * HEAD], 2)

        return [functools.partial(job, c) for c in range(3)]

    def out_jobs(p, last=False):
        def job(m):
            cols = slice(m * 256, (m + 1) * 256)
            slot = place(p) + m // 4
            y = y_s[:, cols] + jnp.dot(o_s[...], w_v[slot, m % 4 * DEEP : (m % 4 + 1) * DEEP, :], preferred_element_type=F32)
            if last:
                out_v[:, cols] = y.astype(BF16)
            else:
                y_s[:, cols] = y

        return [functools.partial(job, m) for m in range(12)]

    strips = [(i, g) for i in range(2) for g in range(GROUP)]
    half = T // 2

    def row(p, i, g):
        return 2 * GROUP * p + GROUP * i + g

    def with_ones(v):
        return jnp.concatenate([v, jnp.ones((8, v.shape[1]), BF16)], 0)

    def staged(stages, jobs=()):
        scores, weigh, mix = stages
        count, done, s, w = len(strips), 0, {}, {}
        for at in range(count + 2):
            if at < count:
                s[at] = scores(*strips[at])
            upto = len(jobs) * (at + 1) // (count + 2)
            for job in jobs[done:upto]:
                job()
            done = upto
            if 0 <= at - 1 < count:
                w[at - 1] = weigh(*strips[at - 1], s.pop(at - 1))
            if 0 <= at - 2 < count:
                mix(*strips[at - 2], w.pop(at - 2))

    def own(p):
        seen = lax.broadcasted_iota(jnp.int32, (half, half), 0) <= lax.broadcasted_iota(jnp.int32, (half, half), 1)

        def scores(i, g):
            k, q = k_s.at[me, 2 * p + i], q_s.at[row(p, i, g)]
            return _dot(k[:half], q[:half], 1, 1), _dot(k[...], q[half:], 1, 1)

        def weigh(i, g, s):
            n, (sa, sb) = row(p, i, g), s
            sa = jnp.where(seen, sa, -jnp.inf)
            sb = jnp.concatenate([sb[:half], jnp.where(seen, sb[half:], -jnp.inf)], 0)
            ta, tb = sa.max(0, keepdims=True), sb.max(0, keepdims=True)
            top_s[n, :, :half] = ta
            top_s[n, :, half:] = tb
            return jnp.exp2(sa - ta).astype(BF16), jnp.exp2(sb - tb).astype(BF16)

        def mix(i, g, w):
            n, (wa, wb), v = row(p, i, g), w, with_ones(v_s[me, 2 * p + i])
            mix_s[n, :, :half] = _dot(v[:, :half], wa, 1, 0)
            mix_s[n, :, half:] = _dot(v, wb, 1, 0)

        return scores, weigh, mix

    def full(p, base, srcs, then=None):
        def scores(i, g):
            return [_dot(k_s[src, 2 * p + i], q_s[base + GROUP * i + g], 1, 1) for src in srcs]

        def weigh(i, g, s):
            n = base + GROUP * i + g
            old = top = top_s[n]
            for part in s:
                top = jnp.maximum(top, part.max(0, keepdims=True))
            top_s[n] = top
            return [jnp.exp2(part - top).astype(BF16) for part in s], jnp.exp2(old - top)

        def mix(i, g, w):
            n, (parts, keep) = base + GROUP * i + g, w
            mix_s[n] = mix_s[n] * keep + sum(_dot(with_ones(v_s[src, 2 * p + i]), part, 1, 0) for src, part in zip(srcs, parts))
            if then:
                then(i, g)

        return scores, weigh, mix

    def merge(p):
        for i in range(2 * GROUP):
            a, b = row(p, 0, 0) + i, HEADS + row(p - 2, 0, 0) + i
            top = jnp.maximum(top_s[a], top_s[b])
            mix_s[a] = mix_s[a] * jnp.exp2(top_s[a] - top) + mix_s[b] * jnp.exp2(top_s[b] - top)
            top_s[a] = top

    def finish(p, i, g):
        n, at = row(p, i, g), (GROUP * i + g) * HEAD
        o_s[:, at : at + HEAD] = (mix_s[n, :HEAD] * (1 / mix_s[n, HEAD : HEAD + 1])).astype(BF16).T

    with jax.named_scope("keys_values"):
        for slot in range(3, 9):
            arrive(slot)
        keys_values(range(2, 2 * PAIRS))
        for p in range(1, PAIRS):
            send(p, [0, 1])
        fetch_queries(2, range(3))
        fetch_queries(3, range(3))
    with jax.named_scope("queries"):
        for c in range(3):
            arrive(place(0) + c)
        for job in query_jobs(0):
            job()
        fetch_out(0)

    def take(h):
        for src in range(2):
            for kv in range(2):
                move(src, h, kv, hand_sem.at[kv], me).wait_recv()

                @pl.when(me == 2)
                def _():
                    hand(src, h, kv).start()

    def local(p, _):
        with jax.named_scope("own_queries"):
            for c in range(3):
                arrive(place(p + 1) + c)
            staged(own(p), query_jobs(p + 1))
            fetch_out(p + 1)

        @pl.when(odd & (p >= 1))
        def _():
            lend(p - 1, me - 1).start()

    lax.fori_loop(0, PAIRS - 1, local, None)
    @pl.when(me == 2)
    def _():
        take(0)
        take(1)

    with jax.named_scope("own"):
        staged(own(PAIRS - 1))

    def neighbour(j, _):
        @pl.when(odd)
        def _():
            for i in range(2):
                for kv in range(2):
                    move(me - 1, 2 * j + i, kv, near_sem.at[kv], me).wait_recv()

        @pl.when(even)
        def _():
            lend(j, me).wait_recv()

            @pl.when((me == 2) & (j == 1))
            def _():
                take(2)
                take(3)

            for i in range(2 * GROUP):
                n = HEADS + 2 * GROUP * j + i
                top_s[n] = jnp.full((1, T), NEG, F32)
                mix_s[n] = jnp.zeros((HEAD + 8, T), F32)

        with jax.named_scope("neighbour"):
            base = 2 * GROUP * j + jnp.where(odd, 0, HEADS)
            staged(full(j + jnp.where(odd, 0, 2), base, (me - lax.rem(me, 2),)))

        @pl.when(even)
        def _():
            for c in give(j, me + 1):
                c.start()

    lax.fori_loop(0, 2, neighbour, None)

    for n in range(SLOTS):
        arrive(n)

    def remote(p, _):
        @pl.when(odd & (p >= 2))
        def _():
            with jax.named_scope("merge"):
                for c in give(p - 2, me):
                    c.wait_recv()
                merge(p)

        @pl.when(me >= 2)
        def _():
            with jax.named_scope("linked_wait"):

                @pl.when(me == 3)
                def _():
                    take(2 * p)
                    take(2 * p + 1)

            with jax.named_scope("linked"):
                staged(full(p, row(p, 0, 0), (0, 1), functools.partial(finish, p)))

        @pl.when((me == 2) & (p == 1))
        def _():
            take(4)
            take(5)

        @pl.when((me == 2) & (p == 2))
        def _():
            take(6)
            take(7)

        @pl.when(me < 2)
        def _():
            with jax.named_scope("finish"):
                for i, g in strips:
                    finish(p, i, g)

        @pl.when(p < PAIRS - 1)
        def _():
            with jax.named_scope("out"):
                for job in out_jobs(p):
                    job()

    lax.fori_loop(0, PAIRS, remote, None)
    with jax.named_scope("last_out"):
        for job in out_jobs(PAIRS - 1, True):
            job()

    def left(part, sem):
        pltpu.make_async_remote_copy(part, part, sem, recv_sem.at[0, 0, 0], device_id={"sp": lax.rem(me + 1, 4)}, device_id_type=MESH).wait_send()

    @pl.when(me < 2)
    def _():
        for kv, buf in enumerate((k_s, v_s)):
            left(buf.at[me], link_sem.at[kv])

    @pl.when(even)
    def _():
        for kv, buf in enumerate((k_s, v_s)):
            left(buf.at[me, pl.ds(0, 4)], near_sem.at[kv])
        for i, buf in enumerate((mix_s, top_s)):
            left(buf.at[pl.ds(HEADS, 4 * GROUP)], give_sem.at[i])

    @pl.when(me == 2)
    def _():
        for kv, buf in enumerate((k_s, v_s)):
            left(buf.at[pl.ds(0, 2)], hand_sem.at[kv])

    @pl.when(odd)
    def _():
        left(q_s.at[pl.ds(HEADS, 4 * GROUP)], lend_sem)


def _store(out_v, out_hbm, sem):
    rows = T // 8
    copies = [pltpu.make_async_copy(out_v.at[pl.ds(i * rows, rows)], out_hbm.at[pl.ds(i * rows, rows)], sem.at[i]) for i in range(8)]
    for c in copies:
        c.start()
    for c in copies:
        c.wait()


def solution(mesh):
    def step(x, gain, wq, wk, wv, wo):
        start = jnp.asarray(_table(np.repeat(np.arange(mesh.shape["sp"]) * T, 8)))
        table = jnp.asarray(_table(np.arange(T)))
        anywhere = pl.BlockSpec(memory_space=pl.ANY)
        dma = pltpu.SemaphoreType.DMA
        out = pl.pallas_call(
            _kernel,
            out_shape=pltpu.VMEM((T, D), BF16),
            in_specs=[anywhere] * 8,
            out_specs=pl.BlockSpec(memory_space=pltpu.VMEM),
            scratch_shapes=[
                pltpu.VMEM((T, D), BF16),
                pltpu.VMEM((D,), BF16),
                pltpu.VMEM((8, HEAD), F32),
                pltpu.VMEM((T, HEAD), F32),
                pltpu.VMEM((4, T, HEAD), F32),
                pltpu.VMEM((SLOTS, D, 256), BF16),
                pltpu.VMEM((HEADS + 4 * GROUP, T, HEAD), BF16),
                pltpu.VMEM((4, KV, T, HEAD), BF16),
                pltpu.VMEM((4, KV, HEAD, T), BF16),
                pltpu.VMEM((HEADS + 4 * GROUP, 1, T), F32),
                pltpu.VMEM((HEADS + 4 * GROUP, HEAD + 8, T), F32),
                pltpu.VMEM((T, DEEP), BF16),
                pltpu.VMEM((T, D), F32),
                dma((4,)), dma((3,)), dma((SLOTS,)),
                dma((2,)), dma((2,)), dma((2,)), dma((4, KV, 2)),
                dma, dma((2,)), dma((2,)), dma((2, 2)),
            ],
            compiler_params=pltpu.CompilerParams(collective_id=0, has_side_effects=True, vmem_limit_bytes=LIMIT),
            name="layer",
        )(x, gain, start, table, wq, wk, wv, wo)
        return pl.pallas_call(
            _store,
            out_shape=jax.ShapeDtypeStruct((T, D), BF16),
            in_specs=[pl.BlockSpec(memory_space=pltpu.VMEM)],
            out_specs=anywhere,
            scratch_shapes=[dma((8,))],
            compiler_params=pltpu.CompilerParams(vmem_limit_bytes=2**20),
            name="store",
        )(out)

    tokens, whole = P(("dp", "sp"), None), P(None, None)
    return jax.shard_map(
        step,
        mesh=mesh,
        in_specs=(tokens, P(None), whole, whole, whole, whole),
        out_specs=tokens,
        check_vma=False,
    )
```

```python
import functools

import jax
import jax.numpy as jnp
import numpy as np
from jax import lax
from jax.experimental import pallas as pl
from jax.experimental.pallas import tpu as pltpu
from jax.sharding import PartitionSpec as P

HEAD = 128
HEADS = 24
KV = 8
D = 3072
T = 512
THETA = 10000
LOG2E = 1.4426950408889634
E = HEAD**-0.5 * LOG2E
NEG = -1e30
PAIRS = KV // 2
GROUP = HEADS // KV
DEEP = 2 * GROUP * HEAD
SLOTS = 12
LIMIT = 67043328 - 17 * 2**20
OVER = 100.0
MESH = pl.DeviceIdType.MESH
F32, BF16 = jnp.float32, jnp.bfloat16


def _dot(a, b, ca, cb):
    return lax.dot_general(a, b, (((ca,), (cb,)), ((), ())), preferred_element_type=F32)


def _table(places):
    half = HEAD // 2
    rate = (np.float32(THETA) ** (-np.arange(half, dtype=np.float32) / np.float32(half))).astype(np.float64)
    angle = np.asarray(places, np.float64)[:, None] * rate
    return np.concatenate([np.cos(angle), np.sin(angle)], 1).astype(np.float32)


def _kernel(x_hbm, gain_hbm, start_hbm, tab_hbm, wq, wk, wv, wo, out_v, over_v, q_s, k_s, v_s, a_v, gain_v, start_v, tab_v, turn_v, w_v, top_s, mix_s, o_s, y_s,
            x_sem, small_sem, w_sem, link_sem, near_sem, hand_sem, recv_sem, lend_sem, lent_sem,
            give_sem, given_sem):
    me = lax.axis_index("sp")

    rows = T // 4
    x_copies = [pltpu.make_async_copy(x_hbm.at[pl.ds(i * rows, rows)], a_v.at[pl.ds(i * rows, rows)], x_sem.at[i]) for i in range(4)]

    def columns(i):
        return pl.ds(i * 256 if isinstance(i, int) else pl.multiple_of(i * 256, 256), 256)

    def weights(w, i, slot):
        return pltpu.make_async_copy(w.at[:, columns(i)], w_v.at[slot], w_sem.at[slot])

    def place(p):
        return (3 * (p - 1) if p else 9) if isinstance(p, int) else jnp.where(p == 0, 9, 3 * (p - 1))

    def fetch_queries(p, cs):
        for c in cs:
            weights(wq, 3 * p + c, place(p) + c).start()

    def fetch_out(p):
        for c in range(3):
            slot = place(p) + c
            for r in range(4):
                rows = pl.ds(p * DEEP if isinstance(p, int) else pl.multiple_of(p * DEEP, DEEP), DEEP)
                pltpu.make_async_copy(wo.at[rows, columns(4 * c + r)], w_v.at[slot, pl.ds(r * DEEP, DEEP)], w_sem.at[slot]).start()

    def arrive(slot):
        weights(wq, 0, slot).wait()

    over_v[...] = jnp.zeros((8, T), F32)

    gain_copy = pltpu.make_async_copy(gain_hbm, gain_v, small_sem.at[0])
    angle_copies = [
        pltpu.make_async_copy(start_hbm.at[pl.ds(me * 8, 8)], start_v, small_sem.at[1]),
        pltpu.make_async_copy(tab_hbm, tab_v, small_sem.at[2]),
    ]
    gain_copy.start()
    for c in x_copies:
        c.start()
    weights(wk, 0, 0).start()
    weights(wv, 0, 1).start()
    for c in angle_copies:
        c.start()

    barrier = pltpu.get_barrier_semaphore()
    for i in range(1, 4):
        pl.semaphore_signal(barrier, inc=1, device_id={"sp": lax.rem(me + i, 4)}, device_id_type=MESH)

    def move(src, h, kv, send, to):
        part = (k_s, v_s)[kv].at[src, h]
        return pltpu.make_async_remote_copy(part, part, send_sem=send, recv_sem=recv_sem.at[src, h, kv], device_id={"sp": to}, device_id_type=MESH)

    def link(h, kv):
        return move(me, h, kv, link_sem.at[kv], 2)

    def near(h, kv):
        return move(me, h, kv, near_sem.at[kv], lax.rem(me + 1, 4))

    def hand(src, h, kv):
        return move(src, h, kv, hand_sem.at[kv], 3)

    odd, even = lax.rem(me, 2) == 1, lax.rem(me, 2) == 0

    def lend(j, to):
        queries = pl.ds(2 * GROUP * (2 + j), 2 * GROUP), pl.ds(HEADS + 2 * GROUP * j, 2 * GROUP)
        return pltpu.make_async_remote_copy(
            q_s.at[queries[0]], q_s.at[queries[1]], lend_sem, lent_sem.at[j], device_id={"sp": to}, device_id_type=MESH
        )

    def give(j, to):
        part = pl.ds(HEADS + 2 * GROUP * j, 2 * GROUP)
        return [
            pltpu.make_async_remote_copy(
                buf.at[part], buf.at[part], give_sem.at[i], given_sem.at[j, i], device_id={"sp": to}, device_id_type=MESH
            )
            for i, buf in enumerate((mix_s, top_s))
        ]

    def send(p, kvs):
        @pl.when(me < 2)
        def _():
            for i in range(2):
                for kv in kvs:
                    link(2 * p + i, kv).start()

        @pl.when(even)
        def _():
            for i in range(2):
                for kv in kvs:
                    near(2 * p + i, kv).start()

    with jax.named_scope("norm"):
        gain_copy.wait()
        for i, c in enumerate(x_copies):
            c.wait()
            here = pl.ds(i * rows, rows)
            total = jnp.zeros((rows, 128), F32)
            for at in range(0, D, 128):
                t = a_v[here, at : at + 128].astype(F32)
                total += t * t
            scale = lax.rsqrt(jnp.sum(total, 1, keepdims=True) * (1 / D) + 1e-6)
            for at in range(0, D, 128):
                t = a_v[here, at : at + 128].astype(F32)
                y_s[here, at : at + 128] = t
                a_v[here, at : at + 128] = (t * scale * gain_v[at : at + 128].astype(F32)).astype(BF16)

        for n in range(2, 2 * PAIRS):
            weights((wk, wv)[n % 2], n // 2, n + 1).start()
        fetch_queries(0, range(3))
        fetch_queries(1, [2])

    def project(slot):
        return jnp.dot(a_v[...], w_v[slot], preferred_element_type=F32).astype(BF16)

    def turned(t, at):
        t = t.astype(F32)
        return (t * turn_v[at] + pltpu.roll(t, HEAD // 2, 1) * turn_v[at + 1]).astype(BF16)

    with jax.named_scope("barrier"):
        pl.semaphore_wait(barrier, 3)

    def make_angles():
        low = lax.broadcasted_iota(jnp.int32, (T, HEAD), 1) < HEAD // 2

        def halves(tab):
            other, first = pltpu.roll(tab, HEAD // 2, 1), low[: tab.shape[0]]
            return jnp.where(first, tab, other), jnp.where(first, other, tab)

        (ca, sa), (cb, sb) = halves(start_v[...]), halves(tab_v[...])
        ca, sa = ca[:1], sa[:1]
        cos, sin = ca * cb - sa * sb, sa * cb + ca * sb
        sin = jnp.where(low, -sin, sin)
        for i, t in enumerate((cos, sin, cos * E, sin * E)):
            turn_v[i] = t

    def keys_values(blocks):
        for n in blocks:
            t = project(n if n < 2 else n + 1)
            if n == 0:
                make_angles()
            for i in range(2):
                head = t[:, i * HEAD : (i + 1) * HEAD]
                if n % 2 == 0:
                    k_s[me, n + i] = turned(head, 0)
                else:
                    v_s[me, n - 1 + i] = head.T

    with jax.named_scope("first_keys"):
        for c in angle_copies:
            c.wait()
        arrive(0)
        keys_values([0])
        send(0, [0])
    with jax.named_scope("first_values"):
        arrive(1)
        keys_values([1])
        send(0, [1])
        fetch_queries(1, [0, 1])

    def query_jobs(p):
        def job(c):
            i = 3 * p + c
            q = project(place(p) + c)
            for n in range(2):
                q_s[2 * i + n] = turned(q[:, n * HEAD : (n + 1) * HEAD], 2)

        return [functools.partial(job, c) for c in range(3)]

    def out_jobs(p, last=False):
        def job(m):
            cols = slice(m * 256, (m + 1) * 256)
            slot = place(p) + m // 4
            y = y_s[:, cols] + jnp.dot(o_s[...], w_v[slot, m % 4 * DEEP : (m % 4 + 1) * DEEP, :], preferred_element_type=F32)
            if last:
                out_v[:, cols] = y.astype(BF16)
            else:
                y_s[:, cols] = y

        return [functools.partial(job, m) for m in range(12)]

    strips = [(i, g) for i in range(2) for g in range(GROUP)]
    half = T // 2

    def row(p, i, g):
        return 2 * GROUP * p + GROUP * i + g

    def with_ones(v):
        return jnp.concatenate([v, jnp.ones((8, v.shape[1]), BF16)], 0)

    def staged(stages, jobs=()):
        scores, weigh, mix = stages
        count, done, s, w = len(strips), 0, {}, {}
        for at in range(count + 2):
            if at < count:
                s[at] = scores(*strips[at])
            upto = len(jobs) * (at + 1) // (count + 2)
            for job in jobs[done:upto]:
                job()
            done = upto
            if 0 <= at - 1 < count:
                w[at - 1] = weigh(*strips[at - 1], s.pop(at - 1))
            if 0 <= at - 2 < count:
                mix(*strips[at - 2], w.pop(at - 2))

    def own(p):
        seen = lax.broadcasted_iota(jnp.int32, (half, half), 0) <= lax.broadcasted_iota(jnp.int32, (half, half), 1)

        def scores(i, g):
            k, q = k_s.at[me, 2 * p + i], q_s.at[row(p, i, g)]
            return _dot(k[:half], q[:half], 1, 1), _dot(k[...], q[half:], 1, 1)

        def weigh(i, g, s):
            n, (sa, sb) = row(p, i, g), s
            sa = jnp.where(seen, sa, -jnp.inf)
            sb = jnp.concatenate([sb[:half], jnp.where(seen, sb[half:], -jnp.inf)], 0)
            ta, tb = sa.max(0, keepdims=True), sb.max(0, keepdims=True)
            top_s[n, :, :half] = ta
            top_s[n, :, half:] = tb
            return jnp.exp2(sa - ta).astype(BF16), jnp.exp2(sb - tb).astype(BF16)

        def mix(i, g, w):
            n, (wa, wb), v = row(p, i, g), w, with_ones(v_s[me, 2 * p + i])
            mix_s[n, :, :half] = _dot(v[:, :half], wa, 1, 0)
            mix_s[n, :, half:] = _dot(v, wb, 1, 0)

        return scores, weigh, mix

    def full(p, base, srcs):
        def scores(i, g):
            return [_dot(k_s[src, 2 * p + i], q_s[base + GROUP * i + g], 1, 1) for src in srcs]

        def weigh(i, g, s):
            n = base + GROUP * i + g
            old = top = top_s[n]
            for part in s:
                top = jnp.maximum(top, part.max(0, keepdims=True))
            top_s[n] = top
            return [jnp.exp2(part - top).astype(BF16) for part in s], jnp.exp2(old - top)

        def mix(i, g, w):
            n, (parts, keep) = base + GROUP * i + g, w
            mix_s[n] = mix_s[n] * keep + sum(_dot(with_ones(v_s[src, 2 * p + i]), part, 1, 0) for src, part in zip(srcs, parts))

        return scores, weigh, mix

    def linked(p):
        def scores(i, g):
            return [_dot(k_s[src, 2 * p + i], q_s[row(p, i, g)], 1, 1) for src in range(2)]

        def weigh(i, g, s):
            top = top_s[row(p, i, g)]
            most = functools.reduce(jnp.maximum, [part.reshape(-1, 8, T).max(0) for part in s])
            over_v[...] = jnp.maximum(over_v[...], most - top)
            return [jnp.exp2(part - top).astype(BF16) for part in s]

        def mix(i, g, w):
            total = mix_s[row(p, i, g)] + sum(_dot(with_ones(v_s[src, 2 * p + i]), part, 1, 0) for src, part in enumerate(w))
            finish(i, g, total)

        return scores, weigh, mix

    def merge(p):
        for i in range(2 * GROUP):
            a, b = row(p, 0, 0) + i, HEADS + row(p - 2, 0, 0) + i
            top = jnp.maximum(top_s[a], top_s[b])
            mix_s[a] = mix_s[a] * jnp.exp2(top_s[a] - top) + mix_s[b] * jnp.exp2(top_s[b] - top)
            top_s[a] = top

    def finish(i, g, total):
        at = (GROUP * i + g) * HEAD
        o_s[:, at : at + HEAD] = (total[:HEAD] * (1 / total[HEAD : HEAD + 1])).astype(BF16).T

    with jax.named_scope("keys_values"):
        for slot in range(3, 9):
            arrive(slot)
        keys_values(range(2, 2 * PAIRS))
        for p in range(1, PAIRS):
            send(p, [0, 1])
        fetch_queries(2, range(3))
        fetch_queries(3, range(3))
    with jax.named_scope("queries"):
        for c in range(3):
            arrive(place(0) + c)
        for job in query_jobs(0):
            job()
        fetch_out(0)

    def take(h):
        for src in range(2):
            for kv in range(2):
                move(src, h, kv, hand_sem.at[kv], me).wait_recv()

                @pl.when(me == 2)
                def _():
                    hand(src, h, kv).start()

    def local(p, _):
        with jax.named_scope("own_queries"):
            for c in range(3):
                arrive(place(p + 1) + c)
            staged(own(p), query_jobs(p + 1))
            fetch_out(p + 1)

        @pl.when(odd & (p >= 1))
        def _():
            lend(p - 1, me - 1).start()

    lax.fori_loop(0, PAIRS - 1, local, None)
    @pl.when(me == 2)
    def _():
        take(0)
        take(1)

    with jax.named_scope("own"):
        staged(own(PAIRS - 1))

    def neighbour(j, _):
        @pl.when(odd)
        def _():
            for i in range(2):
                for kv in range(2):
                    move(me - 1, 2 * j + i, kv, near_sem.at[kv], me).wait_recv()

        @pl.when(even)
        def _():
            lend(j, me).wait_recv()

            @pl.when((me == 2) & (j == 1))
            def _():
                take(2)
                take(3)

            for i in range(2 * GROUP):
                n = HEADS + 2 * GROUP * j + i
                top_s[n] = jnp.full((1, T), NEG, F32)
                mix_s[n] = jnp.zeros((HEAD + 8, T), F32)

        with jax.named_scope("neighbour"):
            base = 2 * GROUP * j + jnp.where(odd, 0, HEADS)
            staged(full(j + jnp.where(odd, 0, 2), base, (me - lax.rem(me, 2),)))

        @pl.when(even)
        def _():
            for c in give(j, me + 1):
                c.start()

    lax.fori_loop(0, 2, neighbour, None)

    for n in range(SLOTS):
        arrive(n)

    def remote(p, _):
        @pl.when(odd & (p >= 2))
        def _():
            with jax.named_scope("merge"):
                for c in give(p - 2, me):
                    c.wait_recv()
                merge(p)

        @pl.when(me >= 2)
        def _():
            with jax.named_scope("linked_wait"):

                @pl.when(me == 3)
                def _():
                    take(2 * p)

                @pl.when((me == 3) | (p == PAIRS - 1))
                def _():
                    take(2 * p + 1)

            with jax.named_scope("linked"):
                staged(linked(p))

        @pl.when((me == 2) & (p == 1))
        def _():
            take(4)
            take(5)

        @pl.when((me == 2) & (p == 2))
        def _():
            take(6)

        @pl.when(me < 2)
        def _():
            with jax.named_scope("finish"):
                for i, g in strips:
                    finish(i, g, mix_s[row(p, i, g)])

        @pl.when(p < PAIRS - 1)
        def _():
            with jax.named_scope("out"):
                for job in out_jobs(p):
                    job()

    lax.fori_loop(0, PAIRS, remote, None)
    @pl.when(odd)
    def _():
        for h in range(4, KV):
            for kv in range(2):
                move(me - 1, h, kv, near_sem.at[kv], me).wait_recv()

    with jax.named_scope("last_out"):
        for job in out_jobs(PAIRS - 1, True):
            job()

    def left(part, sem):
        pltpu.make_async_remote_copy(part, part, sem, recv_sem.at[0, 0, 0], device_id={"sp": lax.rem(me + 1, 4)}, device_id_type=MESH).wait_send()

    @pl.when(me < 2)
    def _():
        for kv, buf in enumerate((k_s, v_s)):
            left(buf.at[me], link_sem.at[kv])

    @pl.when(even)
    def _():
        for kv, buf in enumerate((k_s, v_s)):
            left(buf.at[me], near_sem.at[kv])
        for i, buf in enumerate((mix_s, top_s)):
            left(buf.at[pl.ds(HEADS, 4 * GROUP)], give_sem.at[i])

    @pl.when(me == 2)
    def _():
        for kv, buf in enumerate((k_s, v_s)):
            left(buf.at[pl.ds(0, 2)], hand_sem.at[kv])

    @pl.when(odd)
    def _():
        left(q_s.at[pl.ds(HEADS, 4 * GROUP)], lend_sem)


def _store(out_v, over_v, q_s, k_s, v_s, x_hbm, wo, out_hbm, o_v, w_v, x_v, y_v, sem):
    rows = T // 8
    copies = [pltpu.make_async_copy(out_v.at[pl.ds(i * rows, rows)], out_hbm.at[pl.ds(i * rows, rows)], sem.at[i]) for i in range(8)]
    for c in copies:
        c.start()
    zero = jnp.zeros((16, 128), F32)
    for i in range(T // 16):
        for at in range(0, D, 128):
            zero += out_v[i * 16 : (i + 1) * 16, at : at + 128].astype(F32) * 0
    sound = (jnp.max(over_v[...]) <= OVER) & (jnp.sum(zero) == 0)
    for c in copies:
        c.wait()

    @pl.when(jnp.logical_not(sound))
    def _():
        me = lax.axis_index("sp")
        seen = lax.broadcasted_iota(jnp.int32, (T, T), 0) <= lax.broadcasted_iota(jnp.int32, (T, T), 1)

        def head(n, _):
            def block(j, state):
                top, total, mix = state
                src = me - j
                s = _dot(k_s[src, n // GROUP], q_s[n], 1, 1)
                s = jnp.where(seen | (j > 0), s, -jnp.inf)
                new = jnp.maximum(top, s.max(0, keepdims=True))
                w = jnp.exp2(s - new)
                kept = total * jnp.exp2(top - new)
                total = kept + w.sum(0, keepdims=True)
                mix = mix * (kept / total) + _dot(v_s[src, n // GROUP], (w / total).astype(BF16), 1, 0)
                return new, total, mix

            start = jnp.full((1, T), -jnp.inf, F32), jnp.zeros((1, T), F32), jnp.zeros((HEAD, T), F32)
            mix = lax.fori_loop(0, me + 1, block, start)[2]
            o_v[:, pl.ds(pl.multiple_of(n * HEAD, HEAD), HEAD)] = mix.astype(BF16).T

        lax.fori_loop(0, HEADS, head, None)

        def columns(c, _):
            cols = pl.ds(pl.multiple_of(c * 256, 256), 256)
            ins = [pltpu.make_async_copy(wo.at[:, cols], w_v, sem.at[0]), pltpu.make_async_copy(x_hbm.at[:, cols], x_v, sem.at[1])]
            for t in ins:
                t.start()
            for t in ins:
                t.wait()
            y_v[...] = (x_v[...].astype(F32) + jnp.dot(o_v[...], w_v[...], preferred_element_type=F32)).astype(BF16)
            out = pltpu.make_async_copy(y_v, out_hbm.at[:, cols], sem.at[2])
            out.start()
            out.wait()

        lax.fori_loop(0, D // 256, columns, None)


def solution(mesh):
    def step(x, gain, wq, wk, wv, wo):
        start = jnp.asarray(_table(np.repeat(np.arange(mesh.shape["sp"]) * T, 8)))
        table = jnp.asarray(_table(np.arange(T)))
        inside = pl.BlockSpec(memory_space=pltpu.VMEM)
        anywhere = pl.BlockSpec(memory_space=pl.ANY)
        dma = pltpu.SemaphoreType.DMA
        results = pl.pallas_call(
            _kernel,
            out_shape=[
                pltpu.VMEM((T, D), BF16),
                pltpu.VMEM((8, T), F32),
                pltpu.VMEM((HEADS + 4 * GROUP, T, HEAD), BF16),
                pltpu.VMEM((4, KV, T, HEAD), BF16),
                pltpu.VMEM((4, KV, HEAD, T), BF16),
            ],
            in_specs=[anywhere] * 8,
            out_specs=[inside] * 5,
            scratch_shapes=[
                pltpu.VMEM((T, D), BF16),
                pltpu.VMEM((D,), BF16),
                pltpu.VMEM((8, HEAD), F32),
                pltpu.VMEM((T, HEAD), F32),
                pltpu.VMEM((4, T, HEAD), F32),
                pltpu.VMEM((SLOTS, D, 256), BF16),
                pltpu.VMEM((HEADS + 4 * GROUP, 1, T), F32),
                pltpu.VMEM((HEADS + 4 * GROUP, HEAD + 8, T), F32),
                pltpu.VMEM((T, DEEP), BF16),
                pltpu.VMEM((T, D), F32),
                dma((4,)), dma((3,)), dma((SLOTS,)),
                dma((2,)), dma((2,)), dma((2,)), dma((4, KV, 2)),
                dma, dma((2,)), dma((2,)), dma((2, 2)),
            ],
            compiler_params=pltpu.CompilerParams(collective_id=0, has_side_effects=True, vmem_limit_bytes=LIMIT),
            name="layer",
        )(x, gain, start, table, wq, wk, wv, wo)
        return pl.pallas_call(
            _store,
            out_shape=jax.ShapeDtypeStruct((T, D), BF16),
            in_specs=[inside] * 5 + [anywhere] * 2,
            out_specs=anywhere,
            scratch_shapes=[
                pltpu.VMEM((T, D), BF16),
                pltpu.VMEM((D, 256), BF16),
                pltpu.VMEM((T, 256), BF16),
                pltpu.VMEM((T, 256), BF16),
                dma((8,)),
            ],
            compiler_params=pltpu.CompilerParams(vmem_limit_bytes=24 * 2**20),
            name="store",
        )(*results, *(pltpu.with_memory_space_constraint(t, pltpu.HBM) for t in (x, wo)))

    tokens, whole = P(("dp", "sp"), None), P(None, None)
    return jax.shard_map(
        step,
        mesh=mesh,
        in_specs=(tokens, P(None), whole, whole, whole, whole),
        out_specs=tokens,
        check_vma=False,
    )
```

```python
import functools

import jax
import jax.numpy as jnp
import numpy as np
from jax import lax
from jax.experimental import pallas as pl
from jax.experimental.pallas import tpu as pltpu
from jax.sharding import PartitionSpec as P

HEAD = 128
HEADS = 24
KV = 8
D = 3072
T = 512
THETA = 10000
LOG2E = 1.4426950408889634
E = HEAD**-0.5 * LOG2E
NEG = -1e30
PAIRS = KV // 2
GROUP = HEADS // KV
DEEP = 2 * GROUP * HEAD
SLOTS = 12
LIMIT = 67043328 - 17 * 2**20
OVER = 100.0
MESH = pl.DeviceIdType.MESH
F32, BF16 = jnp.float32, jnp.bfloat16


def _dot(a, b, ca, cb):
    return lax.dot_general(a, b, (((ca,), (cb,)), ((), ())), preferred_element_type=F32)


def _table(places):
    half = HEAD // 2
    rate = (np.float32(THETA) ** (-np.arange(half, dtype=np.float32) / np.float32(half))).astype(np.float64)
    angle = np.asarray(places, np.float64)[:, None] * rate
    return np.concatenate([np.cos(angle), np.sin(angle)], 1).astype(np.float32)


def _kernel(x_hbm, gain_hbm, start_hbm, tab_hbm, wq, wk, wv, wo, out_v, over_v, q_s, k_s, v_s, a_v, gain_v, start_v, tab_v, turn_v, w_v, top_s, mix_s, o_s, y_s,
            x_sem, small_sem, w_sem, link_sem, near_sem, hand_sem, recv_sem, lend_sem, lent_sem,
            give_sem, given_sem):
    me = lax.axis_index("sp")

    rows = T // 4
    x_copies = [pltpu.make_async_copy(x_hbm.at[pl.ds(i * rows, rows)], a_v.at[pl.ds(i * rows, rows)], x_sem.at[i]) for i in range(4)]

    def columns(i):
        return pl.ds(i * 256 if isinstance(i, int) else pl.multiple_of(i * 256, 256), 256)

    def weights(w, i, slot):
        return pltpu.make_async_copy(w.at[:, columns(i)], w_v.at[slot], w_sem.at[slot])

    def place(p):
        return (3 * (p - 1) if p else 9) if isinstance(p, int) else jnp.where(p == 0, 9, 3 * (p - 1))

    def fetch_queries(p, cs):
        for c in cs:
            weights(wq, 3 * p + c, place(p) + c).start()

    def fetch_out(p):
        for c in range(3):
            slot = place(p) + c
            for r in range(4):
                rows = pl.ds(p * DEEP if isinstance(p, int) else pl.multiple_of(p * DEEP, DEEP), DEEP)
                pltpu.make_async_copy(wo.at[rows, columns(4 * c + r)], w_v.at[slot, pl.ds(r * DEEP, DEEP)], w_sem.at[slot]).start()

    def arrive(slot):
        weights(wq, 0, slot).wait()

    over_v[...] = jnp.zeros((8, T), F32)

    gain_copy = pltpu.make_async_copy(gain_hbm, gain_v, small_sem.at[0])
    angle_copies = [
        pltpu.make_async_copy(start_hbm.at[pl.ds(me * 8, 8)], start_v, small_sem.at[1]),
        pltpu.make_async_copy(tab_hbm, tab_v, small_sem.at[2]),
    ]
    gain_copy.start()
    for c in x_copies:
        c.start()
    weights(wk, 0, 0).start()
    weights(wv, 0, 1).start()
    for c in angle_copies:
        c.start()

    barrier = pltpu.get_barrier_semaphore()
    for i in range(1, 4):
        pl.semaphore_signal(barrier, inc=1, device_id={"sp": lax.rem(me + i, 4)}, device_id_type=MESH)

    def move(src, h, kv, send, to):
        part = (k_s, v_s)[kv].at[src, h]
        return pltpu.make_async_remote_copy(part, part, send_sem=send, recv_sem=recv_sem.at[src, h, kv], device_id={"sp": to}, device_id_type=MESH)

    def link(h, kv):
        return move(me, h, kv, link_sem.at[kv], 2)

    def near(h, kv):
        return move(me, h, kv, near_sem.at[kv], lax.rem(me + 1, 4))

    def hand(src, h, kv):
        return move(src, h, kv, hand_sem.at[kv], 3)

    odd, even = lax.rem(me, 2) == 1, lax.rem(me, 2) == 0

    def lend(j, to):
        queries = pl.ds(2 * GROUP * (2 + j), 2 * GROUP), pl.ds(HEADS + 2 * GROUP * j, 2 * GROUP)
        return pltpu.make_async_remote_copy(
            q_s.at[queries[0]], q_s.at[queries[1]], lend_sem, lent_sem.at[j], device_id={"sp": to}, device_id_type=MESH
        )

    def give(j, to):
        part = pl.ds(HEADS + 2 * GROUP * j, 2 * GROUP)
        return [
            pltpu.make_async_remote_copy(
                buf.at[part], buf.at[part], give_sem.at[i], given_sem.at[j, i], device_id={"sp": to}, device_id_type=MESH
            )
            for i, buf in enumerate((mix_s, top_s))
        ]

    def send(p, kvs):
        @pl.when(me < 2)
        def _():
            for i in range(2):
                for kv in kvs:
                    link(2 * p + i, kv).start()

        @pl.when(even)
        def _():
            for i in range(2):
                for kv in kvs:
                    near(2 * p + i, kv).start()

    with jax.named_scope("norm"):
        gain_copy.wait()
        for i, c in enumerate(x_copies):
            c.wait()
            here = pl.ds(i * rows, rows)
            total = jnp.zeros((rows, 128), F32)
            for at in range(0, D, 128):
                t = a_v[here, at : at + 128].astype(F32)
                y_s[here, at : at + 128] = t
                total += t * t
            scale = lax.rsqrt(jnp.sum(total, 1, keepdims=True) * (1 / D) + 1e-6)
            for at in range(0, D, 128):
                t = y_s[here, at : at + 128]
                a_v[here, at : at + 128] = (t * scale * gain_v[at : at + 128].astype(F32)).astype(BF16)

        for n in range(2, 2 * PAIRS):
            weights((wk, wv)[n % 2], n // 2, n + 1).start()
        fetch_queries(0, range(3))
        fetch_queries(1, [2])

    def project(slot):
        return jnp.dot(a_v[...], w_v[slot], preferred_element_type=F32).astype(BF16)

    def turned(t, at):
        t = t.astype(F32)
        return (t * turn_v[at] + pltpu.roll(t, HEAD // 2, 1) * turn_v[at + 1]).astype(BF16)

    with jax.named_scope("barrier"):
        pl.semaphore_wait(barrier, 3)

    def make_angles():
        low = lax.broadcasted_iota(jnp.int32, (T, HEAD), 1) < HEAD // 2

        def halves(tab):
            other, first = pltpu.roll(tab, HEAD // 2, 1), low[: tab.shape[0]]
            return jnp.where(first, tab, other), jnp.where(first, other, tab)

        (ca, sa), (cb, sb) = halves(start_v[...]), halves(tab_v[...])
        ca, sa = ca[:1], sa[:1]
        cos, sin = ca * cb - sa * sb, sa * cb + ca * sb
        sin = jnp.where(low, -sin, sin)
        for i, t in enumerate((cos, sin, cos * E, sin * E)):
            turn_v[i] = t

    def keys_values(blocks):
        for n in blocks:
            t = project(n if n < 2 else n + 1)
            if n == 0:
                make_angles()
            for i in range(2):
                head = t[:, i * HEAD : (i + 1) * HEAD]
                if n % 2 == 0:
                    k_s[me, n + i] = turned(head, 0)
                else:
                    v_s[me, n - 1 + i] = head.T

    with jax.named_scope("first_keys"):
        for c in angle_copies:
            c.wait()
        arrive(0)
        keys_values([0])
        send(0, [0])
    with jax.named_scope("first_values"):
        arrive(1)
        keys_values([1])
        send(0, [1])
        fetch_queries(1, [0, 1])

    def query_jobs(p):
        def job(c):
            i = 3 * p + c
            q = project(place(p) + c)
            for n in range(2):
                q_s[2 * i + n] = turned(q[:, n * HEAD : (n + 1) * HEAD], 2)

        return [functools.partial(job, c) for c in range(3)]

    def out_jobs(p, last=False):
        def job(m):
            cols = slice(m * 256, (m + 1) * 256)
            slot = place(p) + m // 4
            y = y_s[:, cols] + jnp.dot(o_s[...], w_v[slot, m % 4 * DEEP : (m % 4 + 1) * DEEP, :], preferred_element_type=F32)
            if last:
                out_v[:, cols] = y.astype(BF16)
            else:
                y_s[:, cols] = y

        return [functools.partial(job, m) for m in range(12)]

    strips = [(i, g) for i in range(2) for g in range(GROUP)]
    half = T // 2

    def row(p, i, g):
        return 2 * GROUP * p + GROUP * i + g

    def with_ones(v):
        return jnp.concatenate([v, jnp.ones((8, v.shape[1]), BF16)], 0)

    def staged(stages, jobs=(), strips=strips):
        scores, weigh, mix = stages
        count, done, s, w = len(strips), 0, {}, {}
        for at in range(count + 2):
            if at < count:
                s[at] = scores(*strips[at])
            upto = len(jobs) * (at + 1) // (count + 2)
            for job in jobs[done:upto]:
                job()
            done = upto
            if 0 <= at - 1 < count:
                w[at - 1] = weigh(*strips[at - 1], s.pop(at - 1))
            if 0 <= at - 2 < count:
                mix(*strips[at - 2], w.pop(at - 2))

    def own(p):
        seen = lax.broadcasted_iota(jnp.int32, (half, half), 0) <= lax.broadcasted_iota(jnp.int32, (half, half), 1)

        def scores(i, g):
            k, q = k_s.at[me, 2 * p + i], q_s.at[row(p, i, g)]
            return _dot(k[:half], q[:half], 1, 1), _dot(k[...], q[half:], 1, 1)

        def weigh(i, g, s):
            n, (sa, sb) = row(p, i, g), s
            sa = jnp.where(seen, sa, -jnp.inf)
            sb = jnp.concatenate([sb[:half], jnp.where(seen, sb[half:], -jnp.inf)], 0)
            ta, tb = sa.max(0, keepdims=True), sb.max(0, keepdims=True)
            top_s[n, :, :half] = ta
            top_s[n, :, half:] = tb
            return jnp.exp2(sa - ta).astype(BF16), jnp.exp2(sb - tb).astype(BF16)

        def mix(i, g, w):
            n, (wa, wb), v = row(p, i, g), w, with_ones(v_s[me, 2 * p + i])
            mix_s[n, :, :half] = _dot(v[:, :half], wa, 1, 0)
            mix_s[n, :, half:] = _dot(v, wb, 1, 0)

        return scores, weigh, mix

    def full(p, base, srcs):
        def scores(i, g):
            return [_dot(k_s[src, 2 * p + i], q_s[base + GROUP * i + g], 1, 1) for src in srcs]

        def weigh(i, g, s):
            n = base + GROUP * i + g
            old = top = top_s[n]
            for part in s:
                top = jnp.maximum(top, part.max(0, keepdims=True))
            top_s[n] = top
            return [jnp.exp2(part - top).astype(BF16) for part in s], jnp.exp2(old - top)

        def mix(i, g, w):
            n, (parts, keep) = base + GROUP * i + g, w
            mix_s[n] = mix_s[n] * keep + sum(_dot(with_ones(v_s[src, 2 * p + i]), part, 1, 0) for src, part in zip(srcs, parts))

        return scores, weigh, mix

    def linked(p):
        def scores(i, g):
            return [_dot(k_s[src, 2 * p + i], q_s[row(p, i, g)], 1, 1) for src in range(2)]

        def weigh(i, g, s):
            top = top_s[row(p, i, g)]
            most = functools.reduce(jnp.maximum, [part.reshape(-1, 8, T).max(0) for part in s])
            over_v[...] = jnp.maximum(over_v[...], most - top)
            return [jnp.exp2(part - top).astype(BF16) for part in s]

        def mix(i, g, w):
            total = mix_s[row(p, i, g)] + sum(_dot(with_ones(v_s[src, 2 * p + i]), part, 1, 0) for src, part in enumerate(w))
            finish(i, g, total)

        return scores, weigh, mix

    def merge(p):
        for i in range(2 * GROUP):
            a, b = row(p, 0, 0) + i, HEADS + row(p - 2, 0, 0) + i
            top = jnp.maximum(top_s[a], top_s[b])
            mix_s[a] = mix_s[a] * jnp.exp2(top_s[a] - top) + mix_s[b] * jnp.exp2(top_s[b] - top)
            top_s[a] = top

    def finish(i, g, total):
        at = (GROUP * i + g) * HEAD
        o_s[:, at : at + HEAD] = (total[:HEAD] * (1 / total[HEAD : HEAD + 1])).astype(BF16).T

    with jax.named_scope("keys_values"):
        for slot in range(3, 9):
            arrive(slot)
        keys_values(range(2, 2 * PAIRS))
        for p in range(1, PAIRS):
            send(p, [0, 1])
        fetch_queries(2, range(3))
        fetch_queries(3, range(3))
    with jax.named_scope("queries"):
        for c in range(3):
            arrive(place(0) + c)
        for job in query_jobs(0):
            job()
        fetch_out(0)

    def take(h):
        for src in range(2):
            for kv in range(2):
                move(src, h, kv, hand_sem.at[kv], me).wait_recv()

                @pl.when(me == 2)
                def _():
                    hand(src, h, kv).start()

    def local(p, _):
        with jax.named_scope("own_queries"):
            for c in range(3):
                arrive(place(p + 1) + c)
            staged(own(p), query_jobs(p + 1))
            fetch_out(p + 1)

        @pl.when(odd & (p >= 1))
        def _():
            lend(p - 1, me - 1).start()

    lax.fori_loop(0, PAIRS - 1, local, None)
    @pl.when(me == 2)
    def _():
        take(0)
        take(1)

    with jax.named_scope("own"):
        staged(own(PAIRS - 1))

    def neighbour(j, _):
        @pl.when(odd)
        def _():
            for i in range(2):
                for kv in range(2):
                    move(me - 1, 2 * j + i, kv, near_sem.at[kv], me).wait_recv()

        @pl.when(even)
        def _():
            lend(j, me).wait_recv()

            @pl.when((me == 2) & (j == 1))
            def _():
                take(2)
                take(3)

            for i in range(2 * GROUP):
                n = HEADS + 2 * GROUP * j + i
                top_s[n] = jnp.full((1, T), NEG, F32)
                mix_s[n] = jnp.zeros((HEAD + 8, T), F32)

        with jax.named_scope("neighbour"):
            base = 2 * GROUP * j + jnp.where(odd, 0, HEADS)
            staged(full(j + jnp.where(odd, 0, 2), base, (me - lax.rem(me, 2),)))

        @pl.when(even)
        def _():
            for c in give(j, me + 1):
                c.start()

    lax.fori_loop(0, 2, neighbour, None)

    for n in range(SLOTS):
        arrive(n)

    def given_back(p):
        with jax.named_scope("merge"):
            for c in give(p - 2, me):
                c.wait_recv()
            merge(p)

    def alone(p):
        @pl.when(me < 2)
        def _():
            with jax.named_scope("finish"):
                for i, g in strips:
                    finish(i, g, mix_s[row(p, i, g)])

    def remote(p, _):
        @pl.when(odd & (p >= 2))
        def _():
            given_back(p)

        @pl.when(me >= 2)
        def _():
            with jax.named_scope("linked_wait"):

                @pl.when(me == 3)
                def _():
                    take(2 * p)
                    take(2 * p + 1)

            with jax.named_scope("linked"):
                staged(linked(p))

        @pl.when((me == 2) & (p == 1))
        def _():
            take(4)
            take(5)

        @pl.when((me == 2) & (p == 2))
        def _():
            take(6)

        alone(p)
        with jax.named_scope("out"):
            for job in out_jobs(p):
                job()

    last = PAIRS - 1
    lax.fori_loop(0, last, remote, None)

    @pl.when(me == 2)
    def _():
        take(KV - 1)

    @pl.when(odd)
    def _():
        given_back(last)

    @pl.when(me >= 2)
    def _():
        @pl.when(me == 3)
        def _():
            take(KV - 2)

        with jax.named_scope("linked_first"):
            staged(linked(last), (), strips[:GROUP])

        @pl.when(me == 3)
        def _():
            take(KV - 1)

        with jax.named_scope("linked_second"):
            staged(linked(last), (), strips[GROUP:])

    alone(last)

    @pl.when(odd)
    def _():
        for h in range(4, KV):
            for kv in range(2):
                move(me - 1, h, kv, near_sem.at[kv], me).wait_recv()

    with jax.named_scope("last_out"):
        for job in out_jobs(PAIRS - 1, True):
            job()

    def left(part, sem):
        pltpu.make_async_remote_copy(part, part, sem, recv_sem.at[0, 0, 0], device_id={"sp": lax.rem(me + 1, 4)}, device_id_type=MESH).wait_send()

    @pl.when(me < 2)
    def _():
        for kv, buf in enumerate((k_s, v_s)):
            left(buf.at[me], link_sem.at[kv])

    @pl.when(even)
    def _():
        for kv, buf in enumerate((k_s, v_s)):
            left(buf.at[me], near_sem.at[kv])
        for i, buf in enumerate((mix_s, top_s)):
            left(buf.at[pl.ds(HEADS, 4 * GROUP)], give_sem.at[i])

    @pl.when(me == 2)
    def _():
        for kv, buf in enumerate((k_s, v_s)):
            left(buf.at[pl.ds(0, 2)], hand_sem.at[kv])

    @pl.when(odd)
    def _():
        left(q_s.at[pl.ds(HEADS, 4 * GROUP)], lend_sem)


def _store(out_v, over_v, q_s, k_s, v_s, x_hbm, wo, out_hbm, o_v, w_v, x_v, y_v, sem):
    rows = T // 8
    copies = [pltpu.make_async_copy(out_v.at[pl.ds(i * rows, rows)], out_hbm.at[pl.ds(i * rows, rows)], sem.at[i]) for i in range(8)]
    for c in copies:
        c.start()
    zero = jnp.zeros((16, 128), F32)
    for i in range(T // 16):
        for at in range(0, D, 128):
            zero += out_v[i * 16 : (i + 1) * 16, at : at + 128].astype(F32) * 0
    sound = (jnp.max(over_v[...]) <= OVER) & (jnp.sum(zero) == 0)
    for c in copies:
        c.wait()

    @pl.when(jnp.logical_not(sound))
    def _():
        me = lax.axis_index("sp")
        seen = lax.broadcasted_iota(jnp.int32, (T, T), 0) <= lax.broadcasted_iota(jnp.int32, (T, T), 1)

        def head(n, _):
            def block(j, state):
                top, total, mix = state
                src = me - j
                s = _dot(k_s[src, n // GROUP], q_s[n], 1, 1)
                s = jnp.where(seen | (j > 0), s, -jnp.inf)
                new = jnp.maximum(top, s.max(0, keepdims=True))
                w = jnp.exp2(s - new)
                kept = total * jnp.exp2(top - new)
                total = kept + w.sum(0, keepdims=True)
                mix = mix * (kept / total) + _dot(v_s[src, n // GROUP], (w / total).astype(BF16), 1, 0)
                return new, total, mix

            start = jnp.full((1, T), -jnp.inf, F32), jnp.zeros((1, T), F32), jnp.zeros((HEAD, T), F32)
            mix = lax.fori_loop(0, me + 1, block, start)[2]
            o_v[:, pl.ds(pl.multiple_of(n * HEAD, HEAD), HEAD)] = mix.astype(BF16).T

        lax.fori_loop(0, HEADS, head, None)

        def columns(c, _):
            cols = pl.ds(pl.multiple_of(c * 256, 256), 256)
            ins = [pltpu.make_async_copy(wo.at[:, cols], w_v, sem.at[0]), pltpu.make_async_copy(x_hbm.at[:, cols], x_v, sem.at[1])]
            for t in ins:
                t.start()
            for t in ins:
                t.wait()
            y_v[...] = (x_v[...].astype(F32) + jnp.dot(o_v[...], w_v[...], preferred_element_type=F32)).astype(BF16)
            out = pltpu.make_async_copy(y_v, out_hbm.at[:, cols], sem.at[2])
            out.start()
            out.wait()

        lax.fori_loop(0, D // 256, columns, None)


def solution(mesh):
    def step(x, gain, wq, wk, wv, wo):
        start = jnp.asarray(_table(np.repeat(np.arange(mesh.shape["sp"]) * T, 8)))
        table = jnp.asarray(_table(np.arange(T)))
        inside = pl.BlockSpec(memory_space=pltpu.VMEM)
        anywhere = pl.BlockSpec(memory_space=pl.ANY)
        dma = pltpu.SemaphoreType.DMA
        results = pl.pallas_call(
            _kernel,
            out_shape=[
                pltpu.VMEM((T, D), BF16),
                pltpu.VMEM((8, T), F32),
                pltpu.VMEM((HEADS + 4 * GROUP, T, HEAD), BF16),
                pltpu.VMEM((4, KV, T, HEAD), BF16),
                pltpu.VMEM((4, KV, HEAD, T), BF16),
            ],
            in_specs=[anywhere] * 8,
            out_specs=[inside] * 5,
            scratch_shapes=[
                pltpu.VMEM((T, D), BF16),
                pltpu.VMEM((D,), BF16),
                pltpu.VMEM((8, HEAD), F32),
                pltpu.VMEM((T, HEAD), F32),
                pltpu.VMEM((4, T, HEAD), F32),
                pltpu.VMEM((SLOTS, D, 256), BF16),
                pltpu.VMEM((HEADS + 4 * GROUP, 1, T), F32),
                pltpu.VMEM((HEADS + 4 * GROUP, HEAD + 8, T), F32),
                pltpu.VMEM((T, DEEP), BF16),
                pltpu.VMEM((T, D), F32),
                dma((4,)), dma((3,)), dma((SLOTS,)),
                dma((2,)), dma((2,)), dma((2,)), dma((4, KV, 2)),
                dma, dma((2,)), dma((2,)), dma((2, 2)),
            ],
            compiler_params=pltpu.CompilerParams(collective_id=0, has_side_effects=True, vmem_limit_bytes=LIMIT),
            name="layer",
        )(x, gain, start, table, wq, wk, wv, wo)
        return pl.pallas_call(
            _store,
            out_shape=jax.ShapeDtypeStruct((T, D), BF16),
            in_specs=[inside] * 5 + [anywhere] * 2,
            out_specs=anywhere,
            scratch_shapes=[
                pltpu.VMEM((T, D), BF16),
                pltpu.VMEM((D, 256), BF16),
                pltpu.VMEM((T, 256), BF16),
                pltpu.VMEM((T, 256), BF16),
                dma((8,)),
            ],
            compiler_params=pltpu.CompilerParams(vmem_limit_bytes=24 * 2**20),
            name="store",
        )(*results, *(pltpu.with_memory_space_constraint(t, pltpu.HBM) for t in (x, wo)))

    tokens, whole = P(("dp", "sp"), None), P(None, None)
    return jax.shard_map(
        step,
        mesh=mesh,
        in_specs=(tokens, P(None), whole, whole, whole, whole),
        out_specs=tokens,
        check_vma=False,
    )
```

```python
import functools

import jax
import jax.numpy as jnp
import numpy as np
from jax import lax
from jax.experimental import pallas as pl
from jax.experimental.pallas import tpu as pltpu
from jax.sharding import PartitionSpec as P

HEAD = 128
HEADS = 24
KV = 8
D = 3072
T = 512
THETA = 10000
LOG2E = 1.4426950408889634
E = HEAD**-0.5 * LOG2E
NEG = -1e30
PAIRS = KV // 2
GROUP = HEADS // KV
DEEP = 2 * GROUP * HEAD
SLOTS = 12
LIMIT = 67043328 - 17 * 2**20
OVER = 100.0
MESH = pl.DeviceIdType.MESH
F32, BF16 = jnp.float32, jnp.bfloat16


def _dot(a, b, ca, cb):
    return lax.dot_general(a, b, (((ca,), (cb,)), ((), ())), preferred_element_type=F32)


def _table(places):
    half = HEAD // 2
    rate = (np.float32(THETA) ** (-np.arange(half, dtype=np.float32) / np.float32(half))).astype(np.float64)
    angle = np.asarray(places, np.float64)[:, None] * rate
    return np.concatenate([np.cos(angle), np.sin(angle)], 1).astype(np.float32)


def _kernel(x_hbm, gain_hbm, start_hbm, tab_hbm, wq, wk, wv, wo, out_v, over_v, q_s, k_s, v_s, a_v, gain_v, start_v, tab_v, turn_v, w_v, top_s, mix_s, o_s, y_s,
            x_sem, small_sem, w_sem, link_sem, near_sem, hand_sem, recv_sem, lend_sem, lent_sem,
            give_sem, given_sem):
    me = lax.axis_index("sp")

    rows = T // 8
    x_copies = [pltpu.make_async_copy(x_hbm.at[pl.ds(i * rows, rows)], a_v.at[pl.ds(i * rows, rows)], x_sem.at[i]) for i in range(8)]

    def columns(i):
        return pl.ds(i * 256 if isinstance(i, int) else pl.multiple_of(i * 256, 256), 256)

    def weights(w, i, slot):
        return pltpu.make_async_copy(w.at[:, columns(i)], w_v.at[slot], w_sem.at[slot])

    def place(p):
        return (3 * (p - 1) if p else 9) if isinstance(p, int) else jnp.where(p == 0, 9, 3 * (p - 1))

    def fetch_queries(p, cs):
        for c in cs:
            weights(wq, 3 * p + c, place(p) + c).start()

    def fetch_out(p):
        for c in range(3):
            slot = place(p) + c
            for r in range(4):
                rows = pl.ds(p * DEEP if isinstance(p, int) else pl.multiple_of(p * DEEP, DEEP), DEEP)
                pltpu.make_async_copy(wo.at[rows, columns(4 * c + r)], w_v.at[slot, pl.ds(r * DEEP, DEEP)], w_sem.at[slot]).start()

    def arrive(slot):
        weights(wq, 0, slot).wait()

    over_v[...] = jnp.zeros((8, T), F32)

    gain_copy = pltpu.make_async_copy(gain_hbm, gain_v, small_sem.at[0])
    angle_copies = [
        pltpu.make_async_copy(start_hbm.at[pl.ds(me * 8, 8)], start_v, small_sem.at[1]),
        pltpu.make_async_copy(tab_hbm, tab_v, small_sem.at[2]),
    ]
    gain_copy.start()
    for c in x_copies:
        c.start()
    weights(wk, 0, 0).start()
    weights(wv, 0, 1).start()
    for c in angle_copies:
        c.start()

    barrier = pltpu.get_barrier_semaphore()
    for i in range(1, 4):
        pl.semaphore_signal(barrier, inc=1, device_id={"sp": lax.rem(me + i, 4)}, device_id_type=MESH)

    def move(src, h, kv, send, to):
        part = (k_s, v_s)[kv].at[src, h]
        return pltpu.make_async_remote_copy(part, part, send_sem=send, recv_sem=recv_sem.at[src, h, kv], device_id={"sp": to}, device_id_type=MESH)

    def link(h, kv):
        return move(me, h, kv, link_sem.at[kv], 2)

    def near(h, kv):
        return move(me, h, kv, near_sem.at[kv], lax.rem(me + 1, 4))

    def hand(src, h, kv):
        return move(src, h, kv, hand_sem.at[kv], 3)

    odd, even = lax.rem(me, 2) == 1, lax.rem(me, 2) == 0

    def lend(j, to):
        queries = pl.ds(2 * GROUP * (2 + j), 2 * GROUP), pl.ds(HEADS + 2 * GROUP * j, 2 * GROUP)
        return pltpu.make_async_remote_copy(
            q_s.at[queries[0]], q_s.at[queries[1]], lend_sem, lent_sem.at[j], device_id={"sp": to}, device_id_type=MESH
        )

    def give(j, to):
        part = pl.ds(HEADS + 2 * GROUP * j, 2 * GROUP)
        return [
            pltpu.make_async_remote_copy(
                buf.at[part], buf.at[part], give_sem.at[i], given_sem.at[j, i], device_id={"sp": to}, device_id_type=MESH
            )
            for i, buf in enumerate((mix_s, top_s))
        ]

    def send(p, kvs):
        @pl.when(me < 2)
        def _():
            for i in range(2):
                for kv in kvs:
                    link(2 * p + i, kv).start()

        @pl.when(even)
        def _():
            for i in range(2):
                for kv in kvs:
                    near(2 * p + i, kv).start()

    with jax.named_scope("norm"):
        gain_copy.wait()
        for i, c in enumerate(x_copies):
            c.wait()
            here = pl.ds(i * rows, rows)
            total = jnp.zeros((rows, 128), F32)
            for at in range(0, D, 128):
                t = a_v[here, at : at + 128].astype(F32)
                y_s[here, at : at + 128] = t
                total += t * t
            scale = lax.rsqrt(jnp.sum(total, 1, keepdims=True) * (1 / D) + 1e-6)
            for at in range(0, D, 128):
                t = y_s[here, at : at + 128]
                a_v[here, at : at + 128] = (t * scale * gain_v[at : at + 128].astype(F32)).astype(BF16)

        for n in range(2, 2 * PAIRS):
            weights((wk, wv)[n % 2], n // 2, n + 1).start()
        fetch_queries(0, range(3))
        fetch_queries(1, [2])

    def project(slot):
        return jnp.dot(a_v[...], w_v[slot], preferred_element_type=F32).astype(BF16)

    def turned(t, at):
        t = t.astype(F32)
        return (t * turn_v[at] + pltpu.roll(t, HEAD // 2, 1) * turn_v[at + 1]).astype(BF16)

    with jax.named_scope("barrier"):
        pl.semaphore_wait(barrier, 3)

    def make_angles():
        low = lax.broadcasted_iota(jnp.int32, (T, HEAD), 1) < HEAD // 2

        def halves(tab):
            other, first = pltpu.roll(tab, HEAD // 2, 1), low[: tab.shape[0]]
            return jnp.where(first, tab, other), jnp.where(first, other, tab)

        (ca, sa), (cb, sb) = halves(start_v[...]), halves(tab_v[...])
        ca, sa = ca[:1], sa[:1]
        cos, sin = ca * cb - sa * sb, sa * cb + ca * sb
        sin = jnp.where(low, -sin, sin)
        for i, t in enumerate((cos, sin, cos * E, sin * E)):
            turn_v[i] = t

    def keys_values(blocks):
        for n in blocks:
            t = project(n if n < 2 else n + 1)
            if n == 0:
                make_angles()
            for i in range(2):
                head = t[:, i * HEAD : (i + 1) * HEAD]
                if n % 2 == 0:
                    k_s[me, n + i] = turned(head, 0)
                else:
                    v_s[me, n - 1 + i] = head.T

    with jax.named_scope("first_keys"):
        for c in angle_copies:
            c.wait()
        arrive(0)
        keys_values([0])
        send(0, [0])
    with jax.named_scope("first_values"):
        arrive(1)
        keys_values([1])
        send(0, [1])
        fetch_queries(1, [0, 1])

    def query_jobs(p):
        def job(c):
            i = 3 * p + c
            q = project(place(p) + c)
            for n in range(2):
                q_s[2 * i + n] = turned(q[:, n * HEAD : (n + 1) * HEAD], 2)

        return [functools.partial(job, c) for c in range(3)]

    def out_jobs(p, last=False):
        def job(m):
            cols = slice(m * 256, (m + 1) * 256)
            slot = place(p) + m // 4
            y = y_s[:, cols] + jnp.dot(o_s[...], w_v[slot, m % 4 * DEEP : (m % 4 + 1) * DEEP, :], preferred_element_type=F32)
            if last:
                out_v[:, cols] = y.astype(BF16)
            else:
                y_s[:, cols] = y

        return [functools.partial(job, m) for m in range(12)]

    strips = [(i, g) for i in range(2) for g in range(GROUP)]
    half = T // 2

    def row(p, i, g):
        return 2 * GROUP * p + GROUP * i + g

    def with_ones(v):
        return jnp.concatenate([v, jnp.ones((8, v.shape[1]), BF16)], 0)

    def staged(stages, jobs=(), strips=strips):
        scores, weigh, mix = stages
        count, done, s, w = len(strips), 0, {}, {}
        for at in range(count + 2):
            if at < count:
                s[at] = scores(*strips[at])
            upto = len(jobs) * (at + 1) // (count + 2)
            for job in jobs[done:upto]:
                job()
            done = upto
            if 0 <= at - 1 < count:
                w[at - 1] = weigh(*strips[at - 1], s.pop(at - 1))
            if 0 <= at - 2 < count:
                mix(*strips[at - 2], w.pop(at - 2))

    def own(p):
        seen = lax.broadcasted_iota(jnp.int32, (half, half), 0) <= lax.broadcasted_iota(jnp.int32, (half, half), 1)

        def scores(i, g):
            k, q = k_s.at[me, 2 * p + i], q_s.at[row(p, i, g)]
            return _dot(k[:half], q[:half], 1, 1), _dot(k[...], q[half:], 1, 1)

        def weigh(i, g, s):
            n, (sa, sb) = row(p, i, g), s
            sa = jnp.where(seen, sa, -jnp.inf)
            sb = jnp.concatenate([sb[:half], jnp.where(seen, sb[half:], -jnp.inf)], 0)
            ta, tb = sa.max(0, keepdims=True), sb.max(0, keepdims=True)
            top_s[n, :, :half] = ta
            top_s[n, :, half:] = tb
            return jnp.exp2(sa - ta).astype(BF16), jnp.exp2(sb - tb).astype(BF16)

        def mix(i, g, w):
            n, (wa, wb), v = row(p, i, g), w, with_ones(v_s[me, 2 * p + i])
            mix_s[n, :, :half] = _dot(v[:, :half], wa, 1, 0)
            mix_s[n, :, half:] = _dot(v, wb, 1, 0)

        return scores, weigh, mix

    def full(p, base, srcs):
        def scores(i, g):
            return [_dot(k_s[src, 2 * p + i], q_s[base + GROUP * i + g], 1, 1) for src in srcs]

        def weigh(i, g, s):
            n = base + GROUP * i + g
            old = top = top_s[n]
            for part in s:
                top = jnp.maximum(top, part.max(0, keepdims=True))
            top_s[n] = top
            return [jnp.exp2(part - top).astype(BF16) for part in s], jnp.exp2(old - top)

        def mix(i, g, w):
            n, (parts, keep) = base + GROUP * i + g, w
            mix_s[n] = mix_s[n] * keep + sum(_dot(with_ones(v_s[src, 2 * p + i]), part, 1, 0) for src, part in zip(srcs, parts))

        return scores, weigh, mix

    def linked(p):
        def scores(i, g):
            return [_dot(k_s[src, 2 * p + i], q_s[row(p, i, g)], 1, 1) for src in range(2)]

        def weigh(i, g, s):
            top = top_s[row(p, i, g)]
            most = functools.reduce(jnp.maximum, [part.reshape(-1, 8, T).max(0) for part in s])
            over_v[...] = jnp.maximum(over_v[...], most - top)
            return [jnp.exp2(part - top).astype(BF16) for part in s]

        def mix(i, g, w):
            total = mix_s[row(p, i, g)] + sum(_dot(with_ones(v_s[src, 2 * p + i]), part, 1, 0) for src, part in enumerate(w))
            finish(i, g, total)

        return scores, weigh, mix

    def merge(p):
        for i in range(2 * GROUP):
            a, b = row(p, 0, 0) + i, HEADS + row(p - 2, 0, 0) + i
            top = jnp.maximum(top_s[a], top_s[b])
            mix_s[a] = mix_s[a] * jnp.exp2(top_s[a] - top) + mix_s[b] * jnp.exp2(top_s[b] - top)
            top_s[a] = top

    def finish(i, g, total):
        at = (GROUP * i + g) * HEAD
        o_s[:, at : at + HEAD] = (total[:HEAD] * (1 / total[HEAD : HEAD + 1])).astype(BF16).T

    with jax.named_scope("keys_values"):
        for slot in range(3, 9):
            arrive(slot)
        keys_values([3, 5, 7, 2, 4, 6])
        for p in range(1, PAIRS):
            send(p, [0, 1])
        fetch_queries(2, range(3))
        fetch_queries(3, range(3))
    with jax.named_scope("queries"):
        for c in range(3):
            arrive(place(0) + c)
        for job in query_jobs(0):
            job()
        fetch_out(0)

    def take(h):
        for src in range(2):
            for kv in range(2):
                move(src, h, kv, hand_sem.at[kv], me).wait_recv()

                @pl.when(me == 2)
                def _():
                    hand(src, h, kv).start()

    def local(p, _):
        with jax.named_scope("own_queries"):
            for c in range(3):
                arrive(place(p + 1) + c)
            staged(own(p), query_jobs(p + 1))
            fetch_out(p + 1)

        @pl.when(odd & (p >= 1))
        def _():
            lend(p - 1, me - 1).start()

    lax.fori_loop(0, PAIRS - 1, local, None)
    @pl.when(me == 2)
    def _():
        take(0)
        take(1)

    with jax.named_scope("own"):
        staged(own(PAIRS - 1))

    def neighbour(j, _):
        @pl.when(odd)
        def _():
            for i in range(2):
                for kv in range(2):
                    move(me - 1, 2 * j + i, kv, near_sem.at[kv], me).wait_recv()

        @pl.when(even)
        def _():
            lend(j, me).wait_recv()

            @pl.when((me == 2) & (j == 1))
            def _():
                take(2)
                take(3)

            for i in range(2 * GROUP):
                n = HEADS + 2 * GROUP * j + i
                top_s[n] = jnp.full((1, T), NEG, F32)
                mix_s[n] = jnp.zeros((HEAD + 8, T), F32)

        with jax.named_scope("neighbour"):
            base = 2 * GROUP * j + jnp.where(odd, 0, HEADS)
            staged(full(j + jnp.where(odd, 0, 2), base, (me - lax.rem(me, 2),)))

        @pl.when(even)
        def _():
            for c in give(j, me + 1):
                c.start()

    lax.fori_loop(0, 2, neighbour, None)

    for n in range(SLOTS):
        arrive(n)

    def given_back(p):
        with jax.named_scope("merge"):
            for c in give(p - 2, me):
                c.wait_recv()
            merge(p)

    def alone(p):
        @pl.when(me < 2)
        def _():
            with jax.named_scope("finish"):
                for i, g in strips:
                    finish(i, g, mix_s[row(p, i, g)])

    def remote(p, _):
        @pl.when(odd & (p >= 2))
        def _():
            given_back(p)

        @pl.when(me >= 2)
        def _():
            with jax.named_scope("linked_wait"):

                @pl.when(me == 3)
                def _():
                    take(2 * p)
                    take(2 * p + 1)

            with jax.named_scope("linked"):
                staged(linked(p))

        @pl.when((me == 2) & (p == 1))
        def _():
            take(4)
            take(5)

        @pl.when((me == 2) & (p == 2))
        def _():
            take(6)

        alone(p)
        with jax.named_scope("out"):
            for job in out_jobs(p):
                job()

    last = PAIRS - 1
    lax.fori_loop(0, last, remote, None)

    @pl.when(me == 2)
    def _():
        take(KV - 1)

    @pl.when(odd)
    def _():
        given_back(last)

    @pl.when(me >= 2)
    def _():
        @pl.when(me == 3)
        def _():
            take(KV - 2)

        with jax.named_scope("linked_first"):
            staged(linked(last), (), strips[:GROUP])

        @pl.when(me == 3)
        def _():
            take(KV - 1)

        with jax.named_scope("linked_second"):
            staged(linked(last), (), strips[GROUP:])

    alone(last)

    @pl.when(odd)
    def _():
        for h in range(4, KV):
            for kv in range(2):
                move(me - 1, h, kv, near_sem.at[kv], me).wait_recv()

    with jax.named_scope("last_out"):
        for job in out_jobs(PAIRS - 1, True):
            job()

    def left(part, sem):
        pltpu.make_async_remote_copy(part, part, sem, recv_sem.at[0, 0, 0], device_id={"sp": lax.rem(me + 1, 4)}, device_id_type=MESH).wait_send()

    @pl.when(me < 2)
    def _():
        for kv, buf in enumerate((k_s, v_s)):
            left(buf.at[me], link_sem.at[kv])

    @pl.when(even)
    def _():
        for kv, buf in enumerate((k_s, v_s)):
            left(buf.at[me], near_sem.at[kv])
        for i, buf in enumerate((mix_s, top_s)):
            left(buf.at[pl.ds(HEADS, 4 * GROUP)], give_sem.at[i])

    @pl.when(me == 2)
    def _():
        for kv, buf in enumerate((k_s, v_s)):
            left(buf.at[pl.ds(0, 2)], hand_sem.at[kv])

    @pl.when(odd)
    def _():
        left(q_s.at[pl.ds(HEADS, 4 * GROUP)], lend_sem)


def _store(out_v, over_v, q_s, k_s, v_s, x_hbm, wo, out_hbm, o_v, w_v, x_v, y_v, sem):
    rows = T // 8
    copies = [pltpu.make_async_copy(out_v.at[pl.ds(i * rows, rows)], out_hbm.at[pl.ds(i * rows, rows)], sem.at[i]) for i in range(8)]
    for c in copies:
        c.start()
    zero = jnp.zeros((16, 128), F32)
    for i in range(T // 16):
        for at in range(0, D, 128):
            zero += out_v[i * 16 : (i + 1) * 16, at : at + 128].astype(F32) * 0
    sound = (jnp.max(over_v[...]) <= OVER) & (jnp.sum(zero) == 0)
    for c in copies:
        c.wait()

    @pl.when(jnp.logical_not(sound))
    def _():
        me = lax.axis_index("sp")
        seen = lax.broadcasted_iota(jnp.int32, (T, T), 0) <= lax.broadcasted_iota(jnp.int32, (T, T), 1)

        def head(n, _):
            def block(j, state):
                top, total, mix = state
                src = me - j
                s = _dot(k_s[src, n // GROUP], q_s[n], 1, 1)
                s = jnp.where(seen | (j > 0), s, -jnp.inf)
                new = jnp.maximum(top, s.max(0, keepdims=True))
                w = jnp.exp2(s - new)
                kept = total * jnp.exp2(top - new)
                total = kept + w.sum(0, keepdims=True)
                mix = mix * (kept / total) + _dot(v_s[src, n // GROUP], (w / total).astype(BF16), 1, 0)
                return new, total, mix

            start = jnp.full((1, T), -jnp.inf, F32), jnp.zeros((1, T), F32), jnp.zeros((HEAD, T), F32)
            mix = lax.fori_loop(0, me + 1, block, start)[2]
            o_v[:, pl.ds(pl.multiple_of(n * HEAD, HEAD), HEAD)] = mix.astype(BF16).T

        lax.fori_loop(0, HEADS, head, None)

        def columns(c, _):
            cols = pl.ds(pl.multiple_of(c * 256, 256), 256)
            ins = [pltpu.make_async_copy(wo.at[:, cols], w_v, sem.at[0]), pltpu.make_async_copy(x_hbm.at[:, cols], x_v, sem.at[1])]
            for t in ins:
                t.start()
            for t in ins:
                t.wait()
            y_v[...] = (x_v[...].astype(F32) + jnp.dot(o_v[...], w_v[...], preferred_element_type=F32)).astype(BF16)
            out = pltpu.make_async_copy(y_v, out_hbm.at[:, cols], sem.at[2])
            out.start()
            out.wait()

        lax.fori_loop(0, D // 256, columns, None)


def solution(mesh):
    def step(x, gain, wq, wk, wv, wo):
        start = jnp.asarray(_table(np.repeat(np.arange(mesh.shape["sp"]) * T, 8)))
        table = jnp.asarray(_table(np.arange(T)))
        inside = pl.BlockSpec(memory_space=pltpu.VMEM)
        anywhere = pl.BlockSpec(memory_space=pl.ANY)
        dma = pltpu.SemaphoreType.DMA
        results = pl.pallas_call(
            _kernel,
            out_shape=[
                pltpu.VMEM((T, D), BF16),
                pltpu.VMEM((8, T), F32),
                pltpu.VMEM((HEADS + 4 * GROUP, T, HEAD), BF16),
                pltpu.VMEM((4, KV, T, HEAD), BF16),
                pltpu.VMEM((4, KV, HEAD, T), BF16),
            ],
            in_specs=[anywhere] * 8,
            out_specs=[inside] * 5,
            scratch_shapes=[
                pltpu.VMEM((T, D), BF16),
                pltpu.VMEM((D,), BF16),
                pltpu.VMEM((8, HEAD), F32),
                pltpu.VMEM((T, HEAD), F32),
                pltpu.VMEM((4, T, HEAD), F32),
                pltpu.VMEM((SLOTS, D, 256), BF16),
                pltpu.VMEM((HEADS + 4 * GROUP, 1, T), F32),
                pltpu.VMEM((HEADS + 4 * GROUP, HEAD + 8, T), F32),
                pltpu.VMEM((T, DEEP), BF16),
                pltpu.VMEM((T, D), F32),
                dma((8,)), dma((3,)), dma((SLOTS,)),
                dma((2,)), dma((2,)), dma((2,)), dma((4, KV, 2)),
                dma, dma((2,)), dma((2,)), dma((2, 2)),
            ],
            compiler_params=pltpu.CompilerParams(collective_id=0, has_side_effects=True, vmem_limit_bytes=LIMIT),
            name="layer",
        )(x, gain, start, table, wq, wk, wv, wo)
        return pl.pallas_call(
            _store,
            out_shape=jax.ShapeDtypeStruct((T, D), BF16),
            in_specs=[inside] * 5 + [anywhere] * 2,
            out_specs=anywhere,
            scratch_shapes=[
                pltpu.VMEM((T, D), BF16),
                pltpu.VMEM((D, 256), BF16),
                pltpu.VMEM((T, 256), BF16),
                pltpu.VMEM((T, 256), BF16),
                dma((8,)),
            ],
            compiler_params=pltpu.CompilerParams(vmem_limit_bytes=24 * 2**20),
            name="store",
        )(*results, *(pltpu.with_memory_space_constraint(t, pltpu.HBM) for t in (x, wo)))

    tokens, whole = P(("dp", "sp"), None), P(None, None)
    return jax.shard_map(
        step,
        mesh=mesh,
        in_specs=(tokens, P(None), whole, whole, whole, whole),
        out_specs=tokens,
        check_vma=False,
    )
```
